32 devices in a mesh: row: 8 (over z, y), col: 4 (over x, core).
Axes of the slice: x: 2, y: 2, z: 4, core: 2. Of those that a mesh axis runs over, the one named last changes fastest.
Arguments:
- spectra: bfloat16 [1024, 16, 128], P(('row', 'col')), may hold values from -4 to 4
- window_flags: int32 [1024, 64], P(('row', 'col')), may hold values 0 or 1
- pair_mask: int32 [1024, 1024], P('row', 'col'), may hold values 0 or 1
- misfit_weight: bfloat16 [16, 1024, 1024], P(None, 'row', 'col'), may hold values from 0.0099487305 to 0.099609375
- observed: bfloat16 [2, 16, 1024, 1024], P(None, None, 'row', 'col'), may hold values from -6 to 6
Outputs:
- grad_first: bfloat16 [1024, 16, 128], P(('row', 'col'))
- grad_second: bfloat16 [4, 256, 16, 128], P('col', 'row')
The draws below stay inside these ranges and needn't reach their ends.
All inputs are finite; a program needn't handle non-finite values. No bound on the sum of `window_flags` or of `pair_mask` on one device may be relied on, other than what follows from the above.
Results may differ from the reference program's by a relative error of at most 0.019.
Values may be sent and summed in bfloat16 or wider, within the bound.
A program may use at most 64 MiB of HBM per device.

```python
import math
import jax
import jax.numpy as jnp
from jax import lax

ROW_BLOCK = 128
FREQS = 16
WINDOWS = 64
STATIONS = 1024
N_ROW = 8
N_COL = 4


def with_ends(values, stream_key, smallest, largest):
    longest = values.shape.index(max(values.shape))
    spots = []
    for shift in (0, 1):
        where = [jax.random.randint(jax.random.fold_in(stream_key, axis), (), 0, length) for axis, length in enumerate(values.shape)]
        where[longest] = (where[longest] + shift) % values.shape[longest]
        spots.append(tuple(where))
    return values.at[spots[0]].set(smallest).at[spots[1]].set(largest)


def levels(stream_key, shape, split, low, high):
    def one(axis_at, parts):
        heights = jax.random.uniform(jax.random.fold_in(jax.random.fold_in(stream_key, 6), axis_at), (parts,), jnp.float32, low / len(split), high / len(split))
        return jnp.repeat(jnp.exp(heights), shape[axis_at] // parts).reshape((-1,) + (1,) * (len(shape) - axis_at - 1))

    gain = one(*split[0])
    for cut in split[1:]:
        gain = gain * one(*cut)
    return gain


def noise(own_key, dims, deviation, bound, pieces=(), held_as=jnp.bfloat16):
    array = jax.random.normal(own_key, dims, jnp.float32) * deviation
    if len(pieces) > 0:
        array = levels(own_key, dims, pieces, -0.22, 0.18) * array
    return jnp.clip(array, min=-bound, max=bound).astype(held_as)


def setup_inputs(seed: int = 0) -> dict:
    seeds = jax.random.split(jax.random.key(seed), 6)
    spectra = noise(seeds[0], (STATIONS, FREQS, 2 * WINDOWS), 0.3, 4.0, ((0, 32),))
    window_flags = with_ends((jax.random.randint(seeds[1], (STATIONS, WINDOWS), 0, 4) < 3).astype(jnp.int32), jax.random.fold_in(seeds[1], 1), 0, 1)
    pair_mask = with_ends((jax.random.randint(seeds[2], (STATIONS, STATIONS), 0, 5) < 3).astype(jnp.int32), jax.random.fold_in(seeds[2], 1), 0, 1)
    misfit_weight = jnp.clip(jnp.exp(math.log(0.099609375) - 2.3038113 * jax.random.uniform(seeds[3], (FREQS, STATIONS, STATIONS), jnp.float32) ** levels(seeds[3], (FREQS, STATIONS, STATIONS), ((1, 8), (2, 4)), -0.2, 0.2)), 0.0099487305, 0.099609375).astype(jnp.bfloat16)
    observed = noise(seeds[4], (2, FREQS, STATIONS, STATIONS), 1.0, 6.0, ((2, 8), (3, 4)))
    return dict(spectra=spectra, window_flags=window_flags, pair_mask=pair_mask, misfit_weight=misfit_weight, observed=observed)


def reference(spectra, window_flags, pair_mask, misfit_weight, observed):
    half_width = spectra.shape[2] // 2
    flag_value = window_flags.astype(jnp.float32)
    flag_both = jnp.concatenate([flag_value, flag_value], axis=1)
    flagged = (spectra.astype(jnp.float32) * flag_both[:, None, :]).astype(jnp.bfloat16)
    flagged_wide = flagged.astype(jnp.float32)
    swapped = jnp.concatenate([-flagged_wide[..., half_width:], flagged_wide[..., :half_width]], axis=-1)
    col_stack = jnp.stack([flagged_wide, swapped])
    row_stack = jnp.stack([flagged_wide, -swapped])
    col_block = STATIONS // N_COL
    mask_wide = pair_mask.astype(jnp.float32)
    weight_wide = misfit_weight.astype(jnp.float32)
    observed_wide = observed.astype(jnp.float32)
    split_col = col_stack.reshape(2, N_COL, col_block, FREQS, 2 * WINDOWS)

    def one_block(accum_second, block_index):
        first_row = (block_index * ROW_BLOCK).astype(jnp.int32)
        row_part = lax.dynamic_slice_in_dim(flagged_wide, first_row, ROW_BLOCK, 0)
        row_pair = lax.dynamic_slice_in_dim(row_stack, first_row, ROW_BLOCK, 1)
        mask_part = lax.dynamic_slice_in_dim(mask_wide, first_row, ROW_BLOCK, 0)
        weight_part = lax.dynamic_slice_in_dim(weight_wide, first_row, ROW_BLOCK, 1)
        observed_part = lax.dynamic_slice_in_dim(observed_wide, first_row, ROW_BLOCK, 2)
        cross_spec = jnp.einsum('ifk,cjfk->cfij', row_part, col_stack, precision=lax.Precision.HIGHEST)
        residual = (mask_part[None, None] * weight_part[None] * (cross_spec - observed_part)).astype(jnp.bfloat16)
        residual = lax.optimization_barrier(residual).astype(jnp.float32)
        split_res = residual.reshape(2, FREQS, ROW_BLOCK, N_COL, col_block)
        first_terms = jnp.einsum('cfinj,cnjfk->nifk', split_res, split_col, precision=lax.Precision.HIGHEST)
        first_terms = lax.optimization_barrier(first_terms.astype(jnp.bfloat16)).astype(jnp.float32)
        first_grad = jnp.sum(first_terms, axis=0).astype(jnp.bfloat16)
        second_terms = jnp.einsum('cfij,cifk->jfk', residual, row_pair, precision=lax.Precision.HIGHEST)
        second_terms = lax.optimization_barrier(second_terms.astype(jnp.bfloat16)).astype(jnp.float32)
        return accum_second + second_terms, first_grad

    initial = jnp.zeros((STATIONS, FREQS, 2 * WINDOWS), jnp.float32)
    accum_second, firsts = lax.scan(one_block, initial, jnp.arange(N_ROW, dtype=jnp.int32))
    grad_first = firsts.reshape(STATIONS, FREQS, 2 * WINDOWS)
    grad_second = accum_second.astype(jnp.bfloat16).reshape(N_COL, col_block, FREQS, 2 * WINDOWS)
    return grad_first, grad_second
```

```python
import functools

import jax
import jax.numpy as jnp
from jax import lax
from jax.experimental import pallas as pl
from jax.experimental.pallas import tpu as pltpu
from jax.sharding import PartitionSpec as P

MESH = pl.DeviceIdType.MESH
GROUP = 2
LAG_Y = 3
LAG_STAGES = (4, 4, 4)
LAG_C, LAG_P = 3, 4
Z_FIRST_FROM, Z_FIRST_TO = 0, 8


def z_first(k, chunks):
    return jnp.logical_and(k * 16 >= Z_FIRST_FROM * chunks, k * 16 < Z_FIRST_TO * chunks)


def z_first_count(chunks):
    return sum(Z_FIRST_FROM * chunks <= k * 16 < Z_FIRST_TO * chunks for k in range(chunks))


def kernel(
    n_row, n_col, chunks, group,
    raw_hbm, flags_hbm, mask_hbm, w_hbm, obs_hbm, out_first, out_second,
    raw, flags, mask, own,
    v1, v2, w_v, obs_v, gf, gf_sum, rc, rx, sums, halves, last, ry, turn_in, thin, thin_in,
    in_sem, own_sem, fs, fr, zs, zr, lz, hy, ys, yr,
    cs, cr, ps, pr, hs, hr, bs, br, us, ur, ts, tr,
):
    ratio = n_row // n_col
    n_z = n_row // ratio
    n_x = n_col // 2
    bits = n_z.bit_length() - 1
    row, col = lax.axis_index("row"), lax.axis_index("col")
    z, y = row // ratio, row % ratio
    x, core = col // 2, col % 2
    shard = own.shape[1]
    first_rows = n_col * shard
    second_rows = ratio * first_rows
    half = own.shape[2] // 2

    def col_at(step):
        return ((x + step) % n_x) * 2 + core

    partner = x * 2 + (1 - core)

    def row_y(step):
        return z * ratio + (y + step) % ratio

    def row_z(step):
        return ((z + step) % n_z) * ratio + y

    def span(k):
        return pl.ds(k * group, group)

    def remote(src, dst, ssem, rsem, to_row, to_col):
        return pltpu.make_async_remote_copy(
            src_ref=src, dst_ref=dst, send_sem=ssem, recv_sem=rsem,
            device_id=(to_row, to_col), device_id_type=MESH,
        )

    def send_f(k, d):
        return remote(own.at[span(k)], v1.at[span(k), col], fs.at[d - 1], fr.at[k], row, (col + d) % n_col)

    def send_z(k, d):
        return remote(own.at[span(k)], v2.at[span(k), y, col], zs.at[d - 1], zr.at[k], row_z(d), z)

    def send_home(k, d):
        return remote(own.at[span(k)], v2.at[span(k), y, col], hy.at[d - 1], yr.at[d - 1, k], row_y(d), z)

    def send_y(k, d):
        src = v2.at[span(k), y]
        return remote(src, src, ys.at[d - 1], yr.at[d - 1, k], row_y(d), col)

    def send_c(k):
        return remote(gf.at[span(k), :, 1 - core], rc.at[span(k)], cs, cr.at[k], row, partner)

    def send_p(k, d):
        return remote(gf_sum.at[span(k), (x + d) % n_x], rx.at[d - 1, span(k)], ps.at[d - 1], pr.at[d - 1, k], row, col_at(d))

    def bit(b):
        return (z // 2**b) % 2

    def row_bit(b):
        return (z + (1 - 2 * bit(b)) * 2**b) * ratio + y

    def send_b(k, b):
        return remote(sums[b].at[span(k), :, 1 - bit(b)], halves[b].at[span(k)], bs.at[b], br.at[b, k], row_bit(b), col)

    def send_h(k, d):
        return remote(last.at[span(k), (y + d) % ratio], ry.at[d - 1, span(k)], hs.at[d - 1], hr.at[d - 1, k], row_y(d), col)

    def send_u(k, d):
        return remote(sums[0].at[span(k), :, :, (y + d) % ratio], turn_in.at[d - 1, span(k)], us.at[d - 1], ur.at[d - 1, k], row_y(d), col)

    def send_t(k, b):
        return remote(thin[b].at[span(k), :, 1 - bit(b)], thin_in[b].at[span(k)], ts.at[b], tr.at[b, k], row_bit(b), col)

    home = z == col

    load_w = pltpu.make_async_copy(w_hbm, w_v, in_sem.at[0])
    load_obs = pltpu.make_async_copy(obs_hbm, obs_v, in_sem.at[1])
    load_own = pltpu.make_async_copy(own, v1.at[:, col], own_sem)
    load_raw = pltpu.make_async_copy(raw_hbm, raw, in_sem.at[2])
    load_flags = pltpu.make_async_copy(flags_hbm, flags, in_sem.at[3])
    load_mask = pltpu.make_async_copy(mask_hbm, mask, in_sem.at[4])
    load_raw.start()
    load_flags.start()

    barrier = pltpu.get_barrier_semaphore()

    def tell(to_row, to_col):
        pl.semaphore_signal(barrier, inc=1, device_id=(to_row, to_col), device_id_type=MESH)

    @pl.when(jnp.logical_not(home))
    def _():
        for j in range(n_col):
            tell(col * ratio + y, j)

    @pl.when(home)
    def _():
        for d in range(1, ratio):
            for j in range(n_col):
                tell(row_y(d), j)

    for b in range(bits):
        tell(row_bit(b), col)
    for d in range(1, ratio):
        tell(row_y(d), col)
    for d in range(1, n_col):
        tell(row, (col + d) % n_col)

    load_raw.wait()
    load_flags.wait()
    load_mask.start()
    load_w.start()
    load_obs.start()
    flag_value = flags[...].astype(jnp.float32)
    flag_both = jnp.concatenate([flag_value, flag_value], axis=1)
    flagged = raw[...].astype(jnp.float32) * flag_both[:, None, :]
    own[...] = jnp.transpose(flagged, (1, 0, 2)).astype(jnp.bfloat16)
    load_own.start()
    pl.semaphore_wait(barrier, n_col - 1 + n_z - 1 + bits + 2 * (ratio - 1))

    @pl.loop(0, chunks)
    def _(k):
        for d in range(n_z - 1, 0, -1):
            send_z(k, d).start()
        for d in range(1, n_col):
            send_f(k, d).start()
        for d in range(1, ratio):
            send_home(k, d).start()

    load_own.wait()

    def wait_first(k):
        got = v1.at[span(k), pl.ds(0, n_col - 1)]
        pltpu.make_async_copy(got, got, fr.at[k]).wait()

    def local_copy(k):
        return pltpu.make_async_copy(v1.at[span(k)], v2.at[span(k), y], lz.at[k])

    lane = lax.broadcasted_iota(jnp.int32, (1, 2 * half), 1)
    low_plus = jnp.where(lane < half, 1.0, -1.0).astype(jnp.float32)

    def compute(f):
        a = v1[f].astype(jnp.float32).reshape(first_rows, 2 * half)
        b = v2[f].astype(jnp.float32).reshape(second_rows, 2 * half).astype(jnp.bfloat16)
        turned = pltpu.roll(a, half, 1) * low_plus
        w = jnp.concatenate([a, turned], axis=0).astype(jnp.bfloat16)
        cross = lax.dot_general(w, b, (((1,), (1,)), ((), ())), preferred_element_type=jnp.float32)
        scale = mask[...].astype(jnp.float32) * w_v[f].astype(jnp.float32)
        res = jnp.concatenate(
            [
                (scale * (cross[:first_rows] - obs_v[0, f].astype(jnp.float32))).astype(jnp.bfloat16),
                (scale * (cross[first_rows:] - obs_v[1, f].astype(jnp.float32))).astype(jnp.bfloat16),
            ],
            axis=0,
        )
        t = jnp.dot(res, b, preferred_element_type=jnp.float32)
        g1 = t[:first_rows] - pltpu.roll(t[first_rows:], half, 1) * low_plus
        gf[f] = g1.reshape(n_x, 2, shard, 2 * half).astype(jnp.bfloat16)
        g2 = lax.dot_general(res, w, (((0,), (0,)), ((), ())), preferred_element_type=jnp.float32)
        sums[0][f] = g2.reshape(n_z // 2, 2, ratio, shard, 2 * half).astype(jnp.bfloat16)

    def wide(ref, *at):
        return ref[at].astype(jnp.float32)

    def second_stage(k, step):
        if step < bits:
            @pl.when(z_first(k, chunks))
            def _():
                send_b(k, step).wait_recv()
                total = wide(sums[step], span(k), slice(None), bit(step)) + wide(halves[step], span(k))
                if step + 1 < bits:
                    sums[step + 1][span(k)] = total.reshape(
                        group, n_z // 2 ** (step + 2), 2, ratio, shard, 2 * half
                    ).astype(jnp.bfloat16)
                    send_b(k, step + 1).start()
                else:
                    last[span(k)] = total[:, 0].astype(jnp.bfloat16)
                    for d in range(1, ratio):
                        send_h(k, d).start()
        else:
            @pl.when(z_first(k, chunks))
            def _():
                total = wide(last, span(k), y)
                for d in range(1, ratio):
                    send_h(k, d).wait_recv()
                    total = total + wide(ry, d - 1, span(k))
                out_second[span(k)] = total.astype(jnp.bfloat16)

        @pl.when(jnp.logical_not(z_first(k, chunks)))
        def _():
            if step == 0:
                total = wide(sums[0], span(k), slice(None), slice(None), y)
                for d in range(1, ratio):
                    send_u(k, d).wait_recv()
                    total = total + wide(turn_in, d - 1, span(k))
            else:
                b = step - 1
                send_t(k, b).wait_recv()
                total = wide(thin[b], span(k), slice(None), bit(b)) + wide(thin_in[b], span(k))
            if step < bits:
                thin[step][span(k)] = total.reshape(
                    group, n_z // 2 ** (step + 1), 2, shard, 2 * half
                ).astype(jnp.bfloat16)
                send_t(k, step).start()
            else:
                out_second[span(k)] = total[:, 0].astype(jnp.bfloat16)

    lag_y = LAG_Y
    lag_c = lag_y + LAG_C
    lag_p = lag_c + LAG_P
    lag_s, at = [], lag_y
    for step in range(bits + 1):
        at = at + LAG_STAGES[min(step, len(LAG_STAGES) - 1)]
        lag_s.append(at)

    @pl.loop(0, chunks + max(lag_s[-1], lag_p))
    def _(it):
        @pl.when(it < chunks)
        def _():
            @pl.when(home)
            def _():
                wait_first(it)
                local_copy(it).start()

            @pl.when(jnp.logical_not(home))
            def _():
                got = v2.at[span(it), y]
                pltpu.make_async_copy(got, got, zr.at[it]).wait()
                for d in range(1, ratio):
                    send_y(it, d).start()

        @pl.when(jnp.logical_and(it >= lag_y, it < chunks + lag_y))
        def _():
            k = it - lag_y

            @pl.when(k == 0)
            def _():
                load_mask.wait()
                load_w.wait()
                load_obs.wait()

            for d in range(1, ratio):
                send_y(k, d).wait_recv()

            @pl.when(home)
            def _():
                local_copy(k).wait()

            @pl.when(jnp.logical_not(home))
            def _():
                wait_first(k)

            for i in range(group):
                compute(k * group + i)

            @pl.when(z_first(k, chunks))
            def _():
                send_b(k, 0).start()

            @pl.when(jnp.logical_not(z_first(k, chunks)))
            def _():
                for d in range(1, ratio):
                    send_u(k, d).start()

            send_c(k).start()

        for step in range(bits + 1):
            @pl.when(jnp.logical_and(it >= lag_s[step], it < chunks + lag_s[step]))
            def _():
                second_stage(it - lag_s[step], step)

        @pl.when(jnp.logical_and(it >= lag_c, it < chunks + lag_c))
        def _():
            k = it - lag_c
            send_c(k).wait_recv()
            total = wide(gf, span(k), slice(None), core) + wide(rc, span(k))
            gf_sum[span(k)] = total.astype(jnp.bfloat16)
            for d in range(1, n_x):
                send_p(k, d).start()

        @pl.when(jnp.logical_and(it >= lag_p, it < chunks + lag_p))
        def _():
            k = it - lag_p
            total = wide(gf_sum, span(k), x)
            for d in range(1, n_x):
                send_p(k, d).wait_recv()
                total = total + wide(rx, d - 1, span(k))
            out_first[span(k)] = total.astype(jnp.bfloat16)

    def sent(ref, sem, count=chunks):
        if count:
            got = ref.at[pl.ds(0, count * group)]
            pltpu.make_async_copy(got, got, sem).wait()

    early = z_first_count(chunks)
    for d in range(1, n_col):
        sent(own, fs.at[d - 1])
    for d in range(1, n_z):
        sent(own, zs.at[d - 1])
    for d in range(1, ratio):
        sent(own, hy.at[d - 1])

        @pl.when(jnp.logical_not(home))
        def _():
            sent(v1, ys.at[d - 1])

        sent(own, hs.at[d - 1], early)
        sent(turn_in.at[d - 1], us.at[d - 1], chunks - early)
    for d in range(1, n_x):
        sent(own, ps.at[d - 1])
    sent(rc, cs)
    for b in range(bits):
        sent(halves[b], bs.at[b], early)
        sent(thin_in[b], ts.at[b], chunks - early)


def turn_kernel(first, second, out_first, out_second):
    for src, dst in ((first, out_first), (second, out_second)):
        dst[...] = jnp.transpose(src[...].astype(jnp.float32), (1, 0, 2)).astype(jnp.bfloat16)


def per_device(n_row, n_col, spectra, window_flags, pair_mask, misfit_weight, observed):
    shard, freqs, width = spectra.shape
    ratio = n_row // n_col
    n_z, n_x = n_row // ratio, n_col // 2
    bits = n_z.bit_length() - 1
    group = GROUP if freqs % GROUP == 0 else 1
    chunks = freqs // group
    bf = jnp.bfloat16
    vm = lambda *shape: pltpu.VMEM(shape, bf)
    dma = lambda *shape: pltpu.SemaphoreType.DMA(shape)
    first, second = pl.pallas_call(
        functools.partial(kernel, n_row, n_col, chunks, group),
        out_shape=[pltpu.VMEM((freqs, shard, width), bf)] * 2,
        in_specs=[
            pl.BlockSpec(memory_space=pl.ANY),
        ] * 5,
        out_specs=[pl.BlockSpec(memory_space=pltpu.VMEM)] * 2,
        scratch_shapes=[
            pltpu.VMEM(spectra.shape, bf),
            pltpu.VMEM(window_flags.shape, window_flags.dtype),
            pltpu.VMEM(pair_mask.shape, pair_mask.dtype),
            vm(freqs, shard, width),
            vm(freqs, n_col, shard, width),
            vm(freqs, ratio, n_col, shard, width),
            pltpu.VMEM(misfit_weight.shape, bf),
            pltpu.VMEM(observed.shape, bf),
            vm(freqs, n_x, 2, shard, width),
            vm(freqs, n_x, shard, width),
            vm(freqs, n_x, shard, width),
            vm(n_x - 1, freqs, shard, width),
            [vm(freqs, n_z // 2 ** (b + 1), 2, ratio, shard, width) for b in range(bits)],
            [vm(freqs, n_z // 2 ** (b + 1), ratio, shard, width) for b in range(bits)],
            vm(freqs, ratio, shard, width),
            vm(ratio - 1, freqs, shard, width),
            vm(ratio - 1, freqs, n_z // 2, 2, shard, width),
            [vm(freqs, n_z // 2 ** (b + 1), 2, shard, width) for b in range(bits)],
            [vm(freqs, n_z // 2 ** (b + 1), shard, width) for b in range(bits)],
            dma(5), pltpu.SemaphoreType.DMA,
            dma(n_col - 1), dma(chunks),
            dma(n_z - 1), dma(chunks), dma(chunks), dma(ratio - 1),
            dma(ratio - 1), dma(ratio - 1, chunks),
            pltpu.SemaphoreType.DMA, dma(chunks),
            dma(n_x - 1), dma(n_x - 1, chunks),
            dma(ratio - 1), dma(ratio - 1, chunks),
            dma(bits), dma(bits, chunks),
            dma(ratio - 1), dma(ratio - 1, chunks),
            dma(bits), dma(bits, chunks),
        ],
        compiler_params=pltpu.CompilerParams(collective_id=0, has_side_effects=True),
        name="adjoint",
    )(spectra, window_flags, pair_mask, misfit_weight, observed)
    first, second = pl.pallas_call(
        turn_kernel,
        out_shape=[jax.ShapeDtypeStruct((shard, freqs, width), bf)] * 2,
        in_specs=[pl.BlockSpec(memory_space=pltpu.VMEM)] * 2,
        out_specs=[pl.BlockSpec(memory_space=pltpu.VMEM)] * 2,
        name="turn",
    )(*(pltpu.with_memory_space_constraint(part, pltpu.VMEM) for part in (first, second)))
    return first, second[None]


def solution(mesh):
    placed = (
        P(("row", "col"), None, None),
        P(("row", "col"), None),
        P("row", "col"),
        P(None, "row", "col"),
        P(None, None, "row", "col"),
    )
    return jax.shard_map(
        functools.partial(per_device, mesh.shape["row"], mesh.shape["col"]),
        mesh=mesh,
        in_specs=placed,
        out_specs=(P(("row", "col"), None, None), P("col", "row", None, None)),
        check_vma=False,
    )
```

```python
import functools

import jax
import jax.numpy as jnp
from jax import lax
from jax.experimental import pallas as pl
from jax.experimental.pallas import tpu as pltpu
from jax.sharding import PartitionSpec as P

MESH = pl.DeviceIdType.MESH
GROUP = 2
LAG_Y = 3
LAG_STAGES = (4, 4, 4)
LAG_C, LAG_P = 3, 4
Z_FIRST = (0, 1, 2, 3)
STRAIGHT = (5, 6, 7)
LAG_F = 0


def among(k, some):
    yes = k < 0
    for one in some:
        yes = jnp.logical_or(yes, k == one)
    return yes


def z_first(k):
    return among(k, Z_FIRST)


def straight(k):
    return among(k, STRAIGHT)


def kernel(
    n_row, n_col, chunks, group,
    raw_hbm, flags_hbm, mask_hbm, w_hbm, obs_hbm, out_first, out_second,
    raw, flags, mask, own,
    v1, v2, w_v, obs_v, gf, gf_sum, rc, rx, sums, got_wide, total_wide, box_wide, last, ry, turn_in, thin, got_thin, total_thin, box_thin, straight_in,
    in_sem, own_sem, fx, xr, fs, fr, fn, zs, zr, lz, hy, ys, yr,
    cs, cr, ps, pr, hs, hr, us, ur, zw, zt, mr, br, ds, dr,
):
    ratio = n_row // n_col
    n_z = n_row // ratio
    n_x = n_col // 2
    row, col = lax.axis_index("row"), lax.axis_index("col")
    z, y = row // ratio, row % ratio
    x, core = col // 2, col % 2
    shard = own.shape[1]
    first_rows = n_col * shard
    second_rows = ratio * first_rows
    half = own.shape[2] // 2

    def col_at(step):
        return ((x + step) % n_x) * 2 + core

    partner = x * 2 + (1 - core)

    def row_y(step):
        return z * ratio + (y + step) % ratio

    def row_z(step):
        return ((z + step) % n_z) * ratio + y

    def span(k):
        return pl.ds(k * group, group)

    def remote(src, dst, ssem, rsem, to_row, to_col):
        return pltpu.make_async_remote_copy(
            src_ref=src, dst_ref=dst, send_sem=ssem, recv_sem=rsem,
            device_id=(to_row, to_col), device_id_type=MESH,
        )

    def send_x(k, d):
        return remote(own.at[span(k)], v1.at[span(k), col], fx.at[d - 1], xr.at[k], row, col_at(d))

    def send_own(k):
        return remote(own.at[span(k)], v1.at[span(k), col], fs, fr.at[k], row, partner)

    def send_on(k, d):
        got = v1.at[span(k), col_at(d)]
        return remote(got, got, fn.at[d - 1], fr.at[k], row, partner)

    def send_z(k, d):
        to_z = jnp.where(d <= z, z - d, d)
        return remote(own.at[span(k)], v2.at[span(k), y, col], zs.at[d - 1], zr.at[k], to_z * ratio + y, z)

    def send_home(k, d):
        return remote(own.at[span(k)], v2.at[span(k), y, col], hy.at[d - 1], yr.at[d - 1, k], row_y(d), z)

    def send_y(k, d):
        src = v2.at[span(k), y]
        return remote(src, src, ys.at[d - 1], yr.at[d - 1, k], row_y(d), col)

    def send_c(k):
        return remote(gf.at[span(k), :, 1 - core], rc.at[span(k)], cs, cr.at[k], row, partner)

    def send_p(k, d):
        return remote(gf_sum.at[span(k), (x + d) % n_x], rx.at[d - 1, span(k)], ps.at[d - 1], pr.at[d - 1, k], row, col_at(d))

    upper = (z // (n_z // 2)) % 2
    outer = z % 2 == upper
    mate = z + 1 - 2 * (z % 2)

    def send_mate(k, d, src, dst, sem):
        at = (z + d) % n_z
        return remote(src.at[span(k), at], dst.at[span(k), at], sem, mr.at[k], mate * ratio + y, col)

    def send_box(k, d, src, dst, sem):
        at = (z + d) % n_z
        return remote(src.at[span(k), at], dst.at[z // 2, span(k)], sem, br.at[k], row_z(d), col)

    def send_h(k, d):
        return remote(last.at[span(k), (y + d) % ratio], ry.at[d - 1, span(k)], hs.at[d - 1], hr.at[d - 1, k], row_y(d), col)

    def send_u(k, d):
        return remote(sums.at[span(k), :, (y + d) % ratio], turn_in.at[d - 1, span(k)], us.at[d - 1], ur.at[d - 1, k], row_y(d), col)

    def send_s(k, d):
        return remote(thin.at[span(k), (z + d) % n_z], straight_in.at[d - 1, span(k)], ds.at[d - 1], dr.at[k], row_z(d), col)

    home = z == col

    load_w = pltpu.make_async_copy(w_hbm, w_v, in_sem.at[0])
    load_obs = pltpu.make_async_copy(obs_hbm, obs_v, in_sem.at[1])
    load_own = pltpu.make_async_copy(own, v1.at[:, col], own_sem)
    load_raw = pltpu.make_async_copy(raw_hbm, raw, in_sem.at[2])
    load_flags = pltpu.make_async_copy(flags_hbm, flags, in_sem.at[3])
    load_mask = pltpu.make_async_copy(mask_hbm, mask, in_sem.at[4])
    load_raw.start()
    load_flags.start()

    barrier = pltpu.get_barrier_semaphore()

    def tell(to_row, to_col):
        pl.semaphore_signal(barrier, inc=1, device_id=(to_row, to_col), device_id_type=MESH)

    @pl.when(jnp.logical_not(home))
    def _():
        for j in range(n_col):
            tell(col * ratio + y, j)

    @pl.when(home)
    def _():
        for d in range(1, ratio):
            for j in range(n_col):
                tell(row_y(d), j)

    for d in range(1, n_z):
        tell(row_z(d), col)
    for d in range(1, ratio):
        tell(row_y(d), col)
    for d in range(1, n_col):
        tell(row, (col + d) % n_col)

    load_raw.wait()
    load_flags.wait()
    load_mask.start()
    load_w.start()
    load_obs.start()
    flag_value = flags[...].astype(jnp.float32)
    flag_both = jnp.concatenate([flag_value, flag_value], axis=1)
    flagged = raw[...].astype(jnp.float32) * flag_both[:, None, :]
    own[...] = jnp.transpose(flagged, (1, 0, 2)).astype(jnp.bfloat16)
    load_own.start()
    pl.semaphore_wait(barrier, n_col - 1 + 2 * (n_z - 1) + 2 * (ratio - 1))

    @pl.loop(0, chunks)
    def _(k):
        for d in range(1, n_x):
            send_x(k, d).start()
        for d in range(n_z - 1, 0, -1):
            @pl.when(d <= z)
            def _():
                send_z(k, d).start()
        for d in range(n_z - 1, 0, -1):
            @pl.when(d > z)
            def _():
                send_z(k, d).start()
        for d in range(1, ratio):
            send_home(k, d).start()
        send_own(k).start()

    load_own.wait()

    def pass_first(k):
        got = v1.at[span(k), pl.ds(0, n_x - 1)]
        pltpu.make_async_copy(got, got, xr.at[k]).wait()
        for d in range(1, n_x):
            send_on(k, d).start()

    def wait_first(k):
        got = v1.at[span(k), pl.ds(0, n_x)]
        pltpu.make_async_copy(got, got, fr.at[k]).wait()

    def local_copy(k):
        return pltpu.make_async_copy(v1.at[span(k)], v2.at[span(k), y], lz.at[k])

    lane = lax.broadcasted_iota(jnp.int32, (1, 2 * half), 1)
    low_plus = jnp.where(lane < half, 1.0, -1.0).astype(jnp.float32)

    def compute(f):
        a = v1[f].astype(jnp.float32).reshape(first_rows, 2 * half)
        b = v2[f].astype(jnp.float32).reshape(second_rows, 2 * half).astype(jnp.bfloat16)
        turned = pltpu.roll(a, half, 1) * low_plus
        w = jnp.concatenate([a, turned], axis=0).astype(jnp.bfloat16)
        cross = lax.dot_general(w, b, (((1,), (1,)), ((), ())), preferred_element_type=jnp.float32)
        scale = mask[...].astype(jnp.float32) * w_v[f].astype(jnp.float32)
        res = jnp.concatenate(
            [
                (scale * (cross[:first_rows] - obs_v[0, f].astype(jnp.float32))).astype(jnp.bfloat16),
                (scale * (cross[first_rows:] - obs_v[1, f].astype(jnp.float32))).astype(jnp.bfloat16),
            ],
            axis=0,
        )
        t = jnp.dot(res, b, preferred_element_type=jnp.float32)
        g1 = t[:first_rows] - pltpu.roll(t[first_rows:], half, 1) * low_plus
        gf[f] = g1.reshape(n_x, 2, shard, 2 * half).astype(jnp.bfloat16)
        g2 = lax.dot_general(res, w, (((0,), (0,)), ((), ())), preferred_element_type=jnp.float32)
        sums[f] = g2.reshape(n_z, ratio, shard, 2 * half).astype(jnp.bfloat16)

    def wide(ref, *at):
        return ref[at].astype(jnp.float32)

    def to_mate(k, src, dst, sem):
        @pl.when(outer)
        def _():
            for d in range(1, n_z):
                send_mate(k, d, src, dst, sem).start()

    def fold(k, src, got, total, box, sem):
        @pl.when(jnp.logical_not(outer))
        def _():
            all_of = got.at[span(k), pl.ds(0, n_z - 1)]
            pltpu.make_async_copy(all_of, all_of, mr.at[k]).wait()
            total[span(k), mate] = src[span(k), mate]
            for d in range(1, n_z):
                at = (mate + d) % n_z
                total[span(k), at] = (wide(src, span(k), at) + wide(got, span(k), at)).astype(jnp.bfloat16)
            for d in range(1, n_z):
                send_box(k, d, total, box, sem).start()

    def unfold(k, src, total, box, put):
        pairs = n_z // 2

        def boxes(count):
            all_of = box.at[pl.ds(0, count), span(k)]
            pltpu.make_async_copy(all_of, all_of, br.at[k]).wait()

        @pl.when(outer)
        def _():
            boxes(pairs)
            out = wide(src, span(k), z)
            for m in range(pairs):
                out = out + wide(box, m, span(k))
            put(out.astype(jnp.bfloat16))

        @pl.when(jnp.logical_not(outer))
        def _():
            if pairs > 1:
                boxes(pairs - 1)
            out = wide(total, span(k), z)
            for m in range(1, pairs):
                out = out + wide(box, (z // 2 + m) % pairs, span(k))
            put(out.astype(jnp.bfloat16))

    def second_stage(k, step):
        plain = jnp.logical_not(jnp.logical_or(z_first(k), straight(k)))

        def put_last(value):
            last[span(k)] = value
            for d in range(1, ratio):
                send_h(k, d).start()

        def put_out(value):
            out_second[span(k)] = value

        @pl.when(z_first(k))
        def _():
            if step == 0:
                fold(k, sums, got_wide, total_wide, box_wide, zw)
            elif step == 1:
                unfold(k, sums, total_wide, box_wide, put_last)
            else:
                total = wide(last, span(k), y)
                for d in range(1, ratio):
                    send_h(k, d).wait_recv()
                    total = total + wide(ry, d - 1, span(k))
                put_out(total.astype(jnp.bfloat16))

        if step == 0:
            @pl.when(jnp.logical_not(z_first(k)))
            def _():
                total = wide(sums, span(k), slice(None), y)
                for d in range(1, ratio):
                    send_u(k, d).wait_recv()
                    total = total + wide(turn_in, d - 1, span(k))
                thin[span(k)] = total.astype(jnp.bfloat16)

                @pl.when(straight(k))
                def _():
                    for d in range(1, n_z):
                        send_s(k, d).start()

                @pl.when(jnp.logical_not(straight(k)))
                def _():
                    to_mate(k, thin, got_thin, zt)
        else:
            @pl.when(plain)
            def _():
                if step == 1:
                    fold(k, thin, got_thin, total_thin, box_thin, zt)
                else:
                    unfold(k, thin, total_thin, box_thin, put_out)

        if step == 1:
            @pl.when(straight(k))
            def _():
                got = straight_in.at[:, span(k)]
                pltpu.make_async_copy(got, got, dr.at[k]).wait()
                total = wide(thin, span(k), z)
                for d in range(1, n_z):
                    total = total + wide(straight_in, d - 1, span(k))
                put_out(total.astype(jnp.bfloat16))

    lag_y = LAG_Y
    lag_c = lag_y + LAG_C
    lag_p = lag_c + LAG_P
    lag_s, at = [], lag_y
    for step in range(3):
        at = at + LAG_STAGES[min(step, len(LAG_STAGES) - 1)]
        lag_s.append(at)

    @pl.loop(0, chunks + max(lag_s[-1], lag_p))
    def _(it):
        @pl.when(it < chunks)
        def _():
            @pl.when(jnp.logical_not(home))
            def _():
                got = v2.at[span(it), y]
                pltpu.make_async_copy(got, got, zr.at[it]).wait()
                for d in range(1, ratio):
                    send_y(it, d).start()

        @pl.when(jnp.logical_and(it >= LAG_F, it < chunks + LAG_F))
        def _():
            pass_first(it - LAG_F)

        @pl.when(jnp.logical_and(it >= lag_y, it < chunks + lag_y))
        def _():
            k = it - lag_y

            @pl.when(k == 0)
            def _():
                load_mask.wait()
                load_w.wait()
                load_obs.wait()

            for d in range(1, ratio):
                send_y(k, d).wait_recv()

            wait_first(k)

            @pl.when(home)
            def _():
                local_copy(k).start()
                local_copy(k).wait()

            for i in range(group):
                compute(k * group + i)

            @pl.when(z_first(k))
            def _():
                to_mate(k, sums, got_wide, zw)

            @pl.when(jnp.logical_not(z_first(k)))
            def _():
                for d in range(1, ratio):
                    send_u(k, d).start()

            send_c(k).start()

        for step in range(3):
            @pl.when(jnp.logical_and(it >= lag_s[step], it < chunks + lag_s[step]))
            def _():
                second_stage(it - lag_s[step], step)

        @pl.when(jnp.logical_and(it >= lag_c, it < chunks + lag_c))
        def _():
            k = it - lag_c
            send_c(k).wait_recv()
            total = wide(gf, span(k), slice(None), core) + wide(rc, span(k))
            gf_sum[span(k)] = total.astype(jnp.bfloat16)
            for d in range(1, n_x):
                send_p(k, d).start()

        @pl.when(jnp.logical_and(it >= lag_p, it < chunks + lag_p))
        def _():
            k = it - lag_p
            total = wide(gf_sum, span(k), x)
            for d in range(1, n_x):
                send_p(k, d).wait_recv()
                total = total + wide(rx, d - 1, span(k))
            out_first[span(k)] = total.astype(jnp.bfloat16)

    def sent(ref, sem, count=chunks):
        if count:
            got = ref.at[pl.ds(0, count * group)]
            pltpu.make_async_copy(got, got, sem).wait()

    early = sum(k in Z_FIRST for k in range(chunks))
    last_ones = sum(k in STRAIGHT for k in range(chunks))
    for d in range(1, n_z):
        sent(own, ds.at[d - 1], last_ones)
    sent(own, fs)
    for d in range(1, n_x):
        sent(own, fx.at[d - 1])
        sent(own, fn.at[d - 1])
    for d in range(1, n_z):
        sent(own, zs.at[d - 1])
    for d in range(1, ratio):
        sent(own, hy.at[d - 1])

        @pl.when(jnp.logical_not(home))
        def _():
            sent(v1, ys.at[d - 1])

        sent(own, hs.at[d - 1], early)
        sent(turn_in.at[d - 1], us.at[d - 1], chunks - early)
    for d in range(1, n_x):
        sent(own, ps.at[d - 1])
    sent(rc, cs)
    sent(got_wide.at[:, pl.ds(0, n_z - 1)], zw, early)
    sent(got_thin.at[:, pl.ds(0, n_z - 1)], zt, chunks - early - last_ones)


def turn_kernel(first, second, out_first, out_second):
    for src, dst in ((first, out_first), (second, out_second)):
        dst[...] = jnp.transpose(src[...].astype(jnp.float32), (1, 0, 2)).astype(jnp.bfloat16)


def per_device(n_row, n_col, spectra, window_flags, pair_mask, misfit_weight, observed):
    shard, freqs, width = spectra.shape
    ratio = n_row // n_col
    n_z, n_x = n_row // ratio, n_col // 2
    group = GROUP if freqs % GROUP == 0 else 1
    chunks = freqs // group
    bf = jnp.bfloat16
    vm = lambda *shape: pltpu.VMEM(shape, bf)
    dma = lambda *shape: pltpu.SemaphoreType.DMA(shape)
    first, second = pl.pallas_call(
        functools.partial(kernel, n_row, n_col, chunks, group),
        out_shape=[pltpu.VMEM((freqs, shard, width), bf)] * 2,
        in_specs=[
            pl.BlockSpec(memory_space=pl.ANY),
        ] * 5,
        out_specs=[pl.BlockSpec(memory_space=pltpu.VMEM)] * 2,
        scratch_shapes=[
            pltpu.VMEM(spectra.shape, bf),
            pltpu.VMEM(window_flags.shape, window_flags.dtype),
            pltpu.VMEM(pair_mask.shape, pair_mask.dtype),
            vm(freqs, shard, width),
            vm(freqs, n_col, shard, width),
            vm(freqs, ratio, n_col, shard, width),
            pltpu.VMEM(misfit_weight.shape, bf),
            pltpu.VMEM(observed.shape, bf),
            vm(freqs, n_x, 2, shard, width),
            vm(freqs, n_x, shard, width),
            vm(freqs, n_x, shard, width),
            vm(n_x - 1, freqs, shard, width),
            vm(freqs, n_z, ratio, shard, width),
            vm(freqs, n_z, ratio, shard, width),
            vm(freqs, n_z, ratio, shard, width),
            vm(n_z // 2, freqs, ratio, shard, width),
            vm(freqs, ratio, shard, width),
            vm(ratio - 1, freqs, shard, width),
            vm(ratio - 1, freqs, n_z, shard, width),
            vm(freqs, n_z, shard, width),
            vm(freqs, n_z, shard, width),
            vm(freqs, n_z, shard, width),
            vm(n_z // 2, freqs, shard, width),
            vm(n_z - 1, freqs, shard, width),
            dma(5), pltpu.SemaphoreType.DMA,
            dma(n_x - 1), dma(chunks), pltpu.SemaphoreType.DMA, dma(chunks), dma(n_x - 1),
            dma(n_z - 1), dma(chunks), dma(chunks), dma(ratio - 1),
            dma(ratio - 1), dma(ratio - 1, chunks),
            pltpu.SemaphoreType.DMA, dma(chunks),
            dma(n_x - 1), dma(n_x - 1, chunks),
            dma(ratio - 1), dma(ratio - 1, chunks),
            dma(ratio - 1), dma(ratio - 1, chunks),
            pltpu.SemaphoreType.DMA, pltpu.SemaphoreType.DMA, dma(chunks), dma(chunks),
            dma(n_z - 1), dma(chunks),
        ],
        compiler_params=pltpu.CompilerParams(collective_id=0, has_side_effects=True),
        name="adjoint",
    )(spectra, window_flags, pair_mask, misfit_weight, observed)
    first, second = pl.pallas_call(
        turn_kernel,
        out_shape=[jax.ShapeDtypeStruct((shard, freqs, width), bf)] * 2,
        in_specs=[pl.BlockSpec(memory_space=pltpu.VMEM)] * 2,
        out_specs=[pl.BlockSpec(memory_space=pltpu.VMEM)] * 2,
        name="turn",
    )(*(pltpu.with_memory_space_constraint(part, pltpu.VMEM) for part in (first, second)))
    return first, second[None]


def solution(mesh):
    placed = (
        P(("row", "col"), None, None),
        P(("row", "col"), None),
        P("row", "col"),
        P(None, "row", "col"),
        P(None, None, "row", "col"),
    )
    return jax.shard_map(
        functools.partial(per_device, mesh.shape["row"], mesh.shape["col"]),
        mesh=mesh,
        in_specs=placed,
        out_specs=(P(("row", "col"), None, None), P("col", "row", None, None)),
        check_vma=False,
    )
```

```python
import functools

import jax
import jax.numpy as jnp
from jax import lax
from jax.experimental import pallas as pl
from jax.experimental.pallas import tpu as pltpu
from jax.sharding import PartitionSpec as P

MESH = pl.DeviceIdType.MESH
GROUP = 2
LAG_Y = 3
LAG_STAGES = (4, 4, 4)
LAG_C, LAG_P = 3, 4
Z_FIRST = (0, 1, 2, 3)
STRAIGHT = (5, 6, 7)
LAG_F = 0
BLOCK = 4


def among(k, some):
    yes = k < 0
    for one in some:
        yes = jnp.logical_or(yes, k == one)
    return yes


def z_first(k):
    return among(k, Z_FIRST)


def straight(k):
    return among(k, STRAIGHT)


def kernel(
    n_row, n_col, chunks, group,
    raw_hbm, flags_hbm, mask_hbm, w_hbm, obs_hbm, out_first, out_second,
    raw, flags, mask, own,
    v1, v2, w_v, obs_v, gf, gf_sum, rc, rx, sums, got_wide, total_wide, box_wide, last, ry, turn_in, thin, got_thin, total_thin, box_thin, straight_in,
    in_sem, own_sem, xr, fs, fr, zs, zr, lz, hy, ys, yr,
    cs, cr, ps, pr, hs, us, ur, zw, zt, mr, br, ds,
):
    ratio = n_row // n_col
    n_z = n_row // ratio
    n_x = n_col // 2
    row, col = lax.axis_index("row"), lax.axis_index("col")
    z, y = row // ratio, row % ratio
    x, core = col // 2, col % 2
    shard = own.shape[1]
    first_rows = n_col * shard
    second_rows = ratio * first_rows
    half = own.shape[2] // 2

    def col_at(step):
        return ((x + step) % n_x) * 2 + core

    partner = x * 2 + (1 - core)

    def row_y(step):
        return z * ratio + (y + step) % ratio

    def row_z(step):
        return ((z + step) % n_z) * ratio + y

    block = BLOCK if chunks % BLOCK == 0 else 1

    def wide_span(b):
        return pl.ds(b * block * group, block * group)

    def span(k):
        return pl.ds(k * group, group)

    def remote(src, dst, ssem, rsem, to_row, to_col):
        return pltpu.make_async_remote_copy(
            src_ref=src, dst_ref=dst, send_sem=ssem, recv_sem=rsem,
            device_id=(to_row, to_col), device_id_type=MESH,
        )

    def send_x(k, d):
        return remote(own.at[span(k)], v1.at[span(k), col], fs, xr.at[k], row, col_at(d))

    def send_own(k):
        return remote(own.at[span(k)], v1.at[span(k), col], fs, fr.at[k], row, partner)

    def send_on(k, d):
        got = v1.at[span(k), col_at(d)]
        return remote(got, got, fs, fr.at[k], row, partner)

    def send_z(k, d):
        to_z = jnp.where(d <= z, z - d, d)
        return remote(own.at[span(k)], v2.at[span(k), y, col], zs, zr.at[k], to_z * ratio + y, z)

    def send_home(k, d):
        return remote(own.at[span(k)], v2.at[span(k), y, col], hy.at[d - 1], yr.at[d - 1, k], row_y(d), z)

    def send_y(k, d):
        src = v2.at[span(k), y]
        return remote(src, src, ys.at[d - 1], yr.at[d - 1, k], row_y(d), col)

    def send_c(k):
        return remote(gf.at[span(k), :, 1 - core], rc.at[span(k)], cs, cr.at[k // block], row, partner)

    def send_p(b, d):
        at = wide_span(b)
        return remote(gf_sum.at[at, (x + d) % n_x], rx.at[d - 1, at], ps.at[d - 1], pr.at[d - 1, b], row, col_at(d))

    upper = (z // (n_z // 2)) % 2
    outer = z % 2 == upper
    mate = z + 1 - 2 * (z % 2)

    def send_mate(k, d, src, dst, sem):
        at = (z + d) % n_z
        return remote(src.at[span(k), at], dst.at[span(k), at], sem, mr.at[k], mate * ratio + y, col)

    def send_box(k, d, src, dst, sem):
        at = (z + d) % n_z
        return remote(src.at[span(k), at], dst.at[z // 2, span(k)], sem, br.at[k], row_z(d), col)

    def send_h(k, d):
        return remote(last.at[span(k), (y + d) % ratio], ry.at[d - 1, span(k)], hs.at[d - 1], ur.at[d - 1, k], row_y(d), col)

    def send_u(k, d):
        return remote(sums.at[span(k), :, (y + d) % ratio], turn_in.at[d - 1, span(k)], us.at[d - 1], ur.at[d - 1, k], row_y(d), col)

    def send_s(k, d):
        return remote(thin.at[span(k), (z + d) % n_z], straight_in.at[d - 1, span(k)], ds, br.at[k], row_z(d), col)

    home = z == col

    load_w = pltpu.make_async_copy(w_hbm, w_v, in_sem.at[0])
    load_obs = pltpu.make_async_copy(obs_hbm, obs_v, in_sem.at[1])
    load_own = pltpu.make_async_copy(own, v1.at[:, col], own_sem)
    load_raw = pltpu.make_async_copy(raw_hbm, raw, in_sem.at[2])
    load_flags = pltpu.make_async_copy(flags_hbm, flags, in_sem.at[3])
    load_mask = pltpu.make_async_copy(mask_hbm, mask, in_sem.at[4])
    load_raw.start()
    load_flags.start()

    barrier = pltpu.get_barrier_semaphore()

    def tell(to_row, to_col):
        pl.semaphore_signal(barrier, inc=1, device_id=(to_row, to_col), device_id_type=MESH)

    @pl.when(jnp.logical_not(home))
    def _():
        for j in range(n_col):
            tell(col * ratio + y, j)

    @pl.when(home)
    def _():
        for d in range(1, ratio):
            for j in range(n_col):
                tell(row_y(d), j)

    for d in range(1, n_z):
        tell(row_z(d), col)
    for d in range(1, ratio):
        tell(row_y(d), col)
    for d in range(1, n_col):
        tell(row, (col + d) % n_col)

    load_raw.wait()
    load_flags.wait()
    load_mask.start()
    load_w.start()
    load_obs.start()
    flag_value = flags[...].astype(jnp.float32)
    flag_both = jnp.concatenate([flag_value, flag_value], axis=1)
    flagged = raw[...].astype(jnp.float32) * flag_both[:, None, :]
    own[...] = jnp.transpose(flagged, (1, 0, 2)).astype(jnp.bfloat16)
    load_own.start()
    pl.semaphore_wait(barrier, n_col - 1 + 2 * (n_z - 1) + 2 * (ratio - 1))

    @pl.loop(0, chunks)
    def _(k):
        for d in range(1, n_x):
            send_x(k, d).start()
        for d in range(n_z - 1, 0, -1):
            @pl.when(d <= z)
            def _():
                send_z(k, d).start()
        for d in range(n_z - 1, 0, -1):
            @pl.when(d > z)
            def _():
                send_z(k, d).start()
        for d in range(1, ratio):
            send_home(k, d).start()
        send_own(k).start()

    load_own.wait()

    def pass_first(k):
        got = v1.at[span(k), pl.ds(0, n_x - 1)]
        pltpu.make_async_copy(got, got, xr.at[k]).wait()
        for d in range(1, n_x):
            send_on(k, d).start()

    def wait_first(k):
        got = v1.at[span(k), pl.ds(0, n_x)]
        pltpu.make_async_copy(got, got, fr.at[k]).wait()

    def local_copy(k):
        return pltpu.make_async_copy(v1.at[span(k)], v2.at[span(k), y], lz)

    lane = lax.broadcasted_iota(jnp.int32, (1, 2 * half), 1)
    low_plus = jnp.where(lane < half, 1.0, -1.0).astype(jnp.float32)

    def compute(f):
        a = v1[f].astype(jnp.float32).reshape(first_rows, 2 * half)
        b = v2[f].astype(jnp.float32).reshape(second_rows, 2 * half).astype(jnp.bfloat16)
        turned = pltpu.roll(a, half, 1) * low_plus
        w = jnp.concatenate([a, turned], axis=0).astype(jnp.bfloat16)
        cross = lax.dot_general(w, b, (((1,), (1,)), ((), ())), preferred_element_type=jnp.float32)
        scale = mask[...].astype(jnp.float32) * w_v[f].astype(jnp.float32)
        res = jnp.concatenate(
            [
                (scale * (cross[:first_rows] - obs_v[0, f].astype(jnp.float32))).astype(jnp.bfloat16),
                (scale * (cross[first_rows:] - obs_v[1, f].astype(jnp.float32))).astype(jnp.bfloat16),
            ],
            axis=0,
        )
        t = jnp.dot(res, b, preferred_element_type=jnp.float32)
        g1 = t[:first_rows] - pltpu.roll(t[first_rows:], half, 1) * low_plus
        gf[f] = g1.reshape(n_x, 2, shard, 2 * half).astype(jnp.bfloat16)
        g2 = lax.dot_general(res, w, (((0,), (0,)), ((), ())), preferred_element_type=jnp.float32)
        sums[f] = g2.reshape(n_z, ratio, shard, 2 * half).astype(jnp.bfloat16)

    def wide(ref, *at):
        return ref[at].astype(jnp.float32)

    def to_mate(k, src, dst, sem):
        @pl.when(outer)
        def _():
            for d in range(1, n_z):
                send_mate(k, d, src, dst, sem).start()

    def fold(k, src, got, total, box, sem):
        @pl.when(jnp.logical_not(outer))
        def _():
            all_of = got.at[span(k), pl.ds(0, n_z - 1)]
            pltpu.make_async_copy(all_of, all_of, mr.at[k]).wait()
            total[span(k), mate] = src[span(k), mate]
            for d in range(1, n_z):
                at = (mate + d) % n_z
                total[span(k), at] = (wide(src, span(k), at) + wide(got, span(k), at)).astype(jnp.bfloat16)
            for d in range(1, n_z):
                send_box(k, d, total, box, sem).start()

    def unfold(k, src, total, box, put):
        pairs = n_z // 2

        def boxes(count):
            all_of = box.at[pl.ds(0, count), span(k)]
            pltpu.make_async_copy(all_of, all_of, br.at[k]).wait()

        @pl.when(outer)
        def _():
            boxes(pairs)
            out = wide(src, span(k), z)
            for m in range(pairs):
                out = out + wide(box, m, span(k))
            put(out.astype(jnp.bfloat16))

        @pl.when(jnp.logical_not(outer))
        def _():
            if pairs > 1:
                boxes(pairs - 1)
            out = wide(total, span(k), z)
            for m in range(1, pairs):
                out = out + wide(box, (z // 2 + m) % pairs, span(k))
            put(out.astype(jnp.bfloat16))

    def second_stage(k, step):
        plain = jnp.logical_not(jnp.logical_or(z_first(k), straight(k)))

        def put_last(value):
            last[span(k)] = value
            for d in range(1, ratio):
                send_h(k, d).start()

        def put_out(value):
            out_second[span(k)] = value

        @pl.when(z_first(k))
        def _():
            if step == 0:
                fold(k, sums, got_wide, total_wide, box_wide, zw)
            elif step == 1:
                unfold(k, sums, total_wide, box_wide, put_last)
            else:
                total = wide(last, span(k), y)
                for d in range(1, ratio):
                    send_h(k, d).wait_recv()
                    total = total + wide(ry, d - 1, span(k))
                put_out(total.astype(jnp.bfloat16))

        if step == 0:
            @pl.when(jnp.logical_not(z_first(k)))
            def _():
                total = wide(sums, span(k), slice(None), y)
                for d in range(1, ratio):
                    send_u(k, d).wait_recv()
                    total = total + wide(turn_in, d - 1, span(k))
                thin[span(k)] = total.astype(jnp.bfloat16)

                @pl.when(straight(k))
                def _():
                    for d in range(1, n_z):
                        send_s(k, d).start()

                @pl.when(jnp.logical_not(straight(k)))
                def _():
                    to_mate(k, thin, got_thin, zt)
        else:
            @pl.when(plain)
            def _():
                if step == 1:
                    fold(k, thin, got_thin, total_thin, box_thin, zt)
                else:
                    unfold(k, thin, total_thin, box_thin, put_out)

        if step == 1:
            @pl.when(straight(k))
            def _():
                got = straight_in.at[:, span(k)]
                pltpu.make_async_copy(got, got, br.at[k]).wait()
                total = wide(thin, span(k), z)
                for d in range(1, n_z):
                    total = total + wide(straight_in, d - 1, span(k))
                put_out(total.astype(jnp.bfloat16))

    lag_y = LAG_Y
    lag_c = lag_y + LAG_C
    lag_p = lag_c + LAG_P
    lag_s, at = [], lag_y
    for step in range(3):
        at = at + LAG_STAGES[min(step, len(LAG_STAGES) - 1)]
        lag_s.append(at)

    def sent(ref, sem, count=chunks):
        if count:
            got = ref.at[pl.ds(0, count * group)]
            pltpu.make_async_copy(got, got, sem).wait()

    early = sum(k in Z_FIRST for k in range(chunks))
    last_ones = sum(k in STRAIGHT for k in range(chunks))

    def gather_sent():
        sent(v1.at[:, pl.ds(0, n_col - 1)], fs)
        pltpu.make_async_copy(straight_in, straight_in, zs).wait()
        for d in range(1, ratio):
            sent(own, hy.at[d - 1])

            @pl.when(jnp.logical_not(home))
            def _():
                sent(v1, ys.at[d - 1])

    def sums_sent():
        sent(rc, cs)
        sent(got_wide.at[:, pl.ds(0, n_z - 1)], zw, early)
        for d in range(1, ratio):
            sent(own, hs.at[d - 1], early)
            sent(turn_in.at[d - 1], us.at[d - 1], chunks - early)

    last_wide = max([k for k in range(chunks) if k in Z_FIRST], default=0)
    sums_done = max(chunks + lag_c, last_wide + lag_s[1] + 1)

    @pl.loop(0, chunks + max(lag_s[-1], lag_p))
    def _(it):
        @pl.when(it == chunks + lag_y + 1)
        def _():
            gather_sent()

        @pl.when(it == sums_done + 1)
        def _():
            sums_sent()

        @pl.when(it < chunks)
        def _():
            @pl.when(jnp.logical_not(home))
            def _():
                got = v2.at[span(it), y]
                pltpu.make_async_copy(got, got, zr.at[it]).wait()
                for d in range(1, ratio):
                    send_y(it, d).start()

        @pl.when(jnp.logical_and(it >= LAG_F, it < chunks + LAG_F))
        def _():
            pass_first(it - LAG_F)

        @pl.when(jnp.logical_and(it >= lag_y, it < chunks + lag_y))
        def _():
            k = it - lag_y

            @pl.when(k == 0)
            def _():
                load_mask.wait()
                load_w.wait()
                load_obs.wait()

            for d in range(1, ratio):
                send_y(k, d).wait_recv()

            wait_first(k)

            @pl.when(home)
            def _():
                local_copy(k).start()
                local_copy(k).wait()

            for i in range(group):
                compute(k * group + i)

            @pl.when(z_first(k))
            def _():
                to_mate(k, sums, got_wide, zw)

            @pl.when(jnp.logical_not(z_first(k)))
            def _():
                for d in range(1, ratio):
                    send_u(k, d).start()

            send_c(k).start()

        for step in range(3):
            @pl.when(jnp.logical_and(it >= lag_s[step], it < chunks + lag_s[step]))
            def _():
                second_stage(it - lag_s[step], step)

        def full_block(lag):
            return jnp.logical_and(jnp.logical_and(it >= lag, it < chunks + lag), (it - lag) % block == block - 1)

        @pl.when(full_block(lag_c))
        def _():
            b = (it - lag_c) // block
            at = wide_span(b)
            got = rc.at[at]
            pltpu.make_async_copy(got, got, cr.at[b]).wait()
            gf_sum[at] = (wide(gf, at, slice(None), core) + wide(rc, at)).astype(jnp.bfloat16)
            for d in range(1, n_x):
                send_p(b, d).start()

        @pl.when(full_block(lag_p))
        def _():
            b = (it - lag_p) // block
            at = wide_span(b)
            total = wide(gf_sum, at, x)
            for d in range(1, n_x):
                send_p(b, d).wait_recv()
                total = total + wide(rx, d - 1, at)
            out_first[at] = total.astype(jnp.bfloat16)

    sent(got_thin.at[:, pl.ds(0, n_z - 1)], zt, chunks - early - last_ones)
    if last_ones:
        all_of = straight_in.at[:, pl.ds(0, last_ones * group)]
        pltpu.make_async_copy(all_of, all_of, ds).wait()
    for d in range(1, n_x):
        sent(own, ps.at[d - 1])


def turn_kernel(first, second, out_first, out_second):
    for src, dst in ((first, out_first), (second, out_second)):
        dst[...] = jnp.transpose(src[...].astype(jnp.float32), (1, 0, 2)).astype(jnp.bfloat16)


def per_device(n_row, n_col, spectra, window_flags, pair_mask, misfit_weight, observed):
    shard, freqs, width = spectra.shape
    ratio = n_row // n_col
    n_z, n_x = n_row // ratio, n_col // 2
    group = GROUP if freqs % GROUP == 0 else 1
    chunks = freqs // group
    bf = jnp.bfloat16
    vm = lambda *shape: pltpu.VMEM(shape, bf)
    dma = lambda *shape: pltpu.SemaphoreType.DMA(shape)
    one = pltpu.SemaphoreType.DMA
    blocks = chunks // BLOCK if chunks % BLOCK == 0 else chunks
    first, second = pl.pallas_call(
        functools.partial(kernel, n_row, n_col, chunks, group),
        out_shape=[pltpu.VMEM((freqs, shard, width), bf)] * 2,
        in_specs=[
            pl.BlockSpec(memory_space=pl.ANY),
        ] * 5,
        out_specs=[pl.BlockSpec(memory_space=pltpu.VMEM)] * 2,
        scratch_shapes=[
            pltpu.VMEM(spectra.shape, bf),
            pltpu.VMEM(window_flags.shape, window_flags.dtype),
            pltpu.VMEM(pair_mask.shape, pair_mask.dtype),
            vm(freqs, shard, width),
            vm(freqs, n_col, shard, width),
            vm(freqs, ratio, n_col, shard, width),
            pltpu.VMEM(misfit_weight.shape, bf),
            pltpu.VMEM(observed.shape, bf),
            vm(freqs, n_x, 2, shard, width),
            vm(freqs, n_x, shard, width),
            vm(freqs, n_x, shard, width),
            vm(n_x - 1, freqs, shard, width),
            vm(freqs, n_z, ratio, shard, width),
            vm(freqs, n_z, ratio, shard, width),
            vm(freqs, n_z, ratio, shard, width),
            vm(n_z // 2, freqs, ratio, shard, width),
            vm(freqs, ratio, shard, width),
            vm(ratio - 1, freqs, shard, width),
            vm(ratio - 1, freqs, n_z, shard, width),
            vm(freqs, n_z, shard, width),
            vm(freqs, n_z, shard, width),
            vm(freqs, n_z, shard, width),
            vm(n_z // 2, freqs, shard, width),
            vm(n_z - 1, freqs, shard, width),
            dma(5), pltpu.SemaphoreType.DMA,
            dma(chunks), one, dma(chunks),
            one, dma(chunks), one, dma(ratio - 1),
            dma(ratio - 1), dma(ratio - 1, chunks),
            one, dma(blocks), dma(n_x - 1), dma(n_x - 1, blocks),
            dma(ratio - 1), dma(ratio - 1), dma(ratio - 1, chunks),
            one, one, dma(chunks), dma(chunks), one,
        ],
        compiler_params=pltpu.CompilerParams(collective_id=0, has_side_effects=True),
        name="adjoint",
    )(spectra, window_flags, pair_mask, misfit_weight, observed)
    first, second = pl.pallas_call(
        turn_kernel,
        out_shape=[jax.ShapeDtypeStruct((shard, freqs, width), bf)] * 2,
        in_specs=[pl.BlockSpec(memory_space=pltpu.VMEM)] * 2,
        out_specs=[pl.BlockSpec(memory_space=pltpu.VMEM)] * 2,
        name="turn",
    )(*(pltpu.with_memory_space_constraint(part, pltpu.VMEM) for part in (first, second)))
    return first, second[None]


def solution(mesh):
    placed = (
        P(("row", "col"), None, None),
        P(("row", "col"), None),
        P("row", "col"),
        P(None, "row", "col"),
        P(None, None, "row", "col"),
    )
    return jax.shard_map(
        functools.partial(per_device, mesh.shape["row"], mesh.shape["col"]),
        mesh=mesh,
        in_specs=placed,
        out_specs=(P(("row", "col"), None, None), P("col", "row", None, None)),
        check_vma=False,
    )
```

```python
import functools

import jax
import jax.numpy as jnp
from jax import lax
from jax.experimental import pallas as pl
from jax.experimental.pallas import tpu as pltpu
from jax.sharding import PartitionSpec as P

MESH = pl.DeviceIdType.MESH
GROUP = 2
LAG_Y = 4
LAG_STAGES = (4, 4, 4)
LAG_C, LAG_P = 3, 4
Z_FIRST = (0, 1, 2, 3)
STRAIGHT = (6, 7)
LAG_F = 0
BLOCK = 4


def among(k, some):
    yes = k < 0
    for one in some:
        yes = jnp.logical_or(yes, k == one)
    return yes


def z_first(k):
    return among(k, Z_FIRST)


def straight(k):
    return among(k, STRAIGHT)


def kernel(
    n_row, n_col, chunks, group,
    raw_hbm, flags_hbm, mask_hbm, w_hbm, obs_hbm, out_first, out_second,
    raw, flags, mask, own,
    v1, v2, w_v, obs_v, gf, gf_sum, rc, rx, sums, got_wide, total_wide, box_wide, last, ry, turn_in, thin, got_thin, total_thin, box_thin, straight_in,
    in_sem, own_sem, xr, fs, fr, zs, zr, lz, hy, ys, yr,
    cs, cr, ps, pr, hs, us, ur, zw, zt, mr, br, ds,
):
    ratio = n_row // n_col
    n_z = n_row // ratio
    n_x = n_col // 2
    row, col = lax.axis_index("row"), lax.axis_index("col")
    z, y = row // ratio, row % ratio
    x, core = col // 2, col % 2
    shard = own.shape[1]
    first_rows = n_col * shard
    second_rows = ratio * first_rows
    half = own.shape[2] // 2

    def col_at(step):
        return ((x + step) % n_x) * 2 + core

    partner = x * 2 + (1 - core)

    def row_y(step):
        return z * ratio + (y + step) % ratio

    def row_z(step):
        return ((z + step) % n_z) * ratio + y

    block = BLOCK if chunks % BLOCK == 0 else 1

    def wide_span(b):
        return pl.ds(b * block * group, block * group)

    def span(k):
        return pl.ds(k * group, group)

    def remote(src, dst, ssem, rsem, to_row, to_col):
        return pltpu.make_async_remote_copy(
            src_ref=src, dst_ref=dst, send_sem=ssem, recv_sem=rsem,
            device_id=(to_row, to_col), device_id_type=MESH,
        )

    def send_x(k, d):
        return remote(own.at[span(k)], v1.at[span(k), col], fs, xr.at[k], row, col_at(d))

    def send_own(k):
        return remote(own.at[span(k)], v1.at[span(k), col], fs, fr.at[k], row, partner)

    def send_on(k, d):
        got = v1.at[span(k), col_at(d)]
        return remote(got, got, fs, fr.at[k], row, partner)

    def send_z(k, d):
        to_z = jnp.where(d <= z, z - d, d)
        return remote(own.at[span(k)], v2.at[span(k), y, col], zs, zr.at[k], to_z * ratio + y, z)

    def send_home(k, d):
        return remote(own.at[span(k)], v2.at[span(k), y, col], hy.at[d - 1], yr.at[d - 1, k], row_y(d), z)

    def send_y(k, d):
        src = v2.at[span(k), y]
        return remote(src, src, ys.at[d - 1], yr.at[d - 1, k], row_y(d), col)

    def send_c(k):
        return remote(gf.at[span(k), :, 1 - core], rc.at[span(k)], cs, cr.at[k // block], row, partner)

    def send_p(b, d):
        at = wide_span(b)
        return remote(gf_sum.at[at, (x + d) % n_x], rx.at[d - 1, at], ps.at[d - 1], pr.at[d - 1, b], row, col_at(d))

    upper = (z // (n_z // 2)) % 2
    outer = z % 2 == upper
    mate = z + 1 - 2 * (z % 2)

    def send_mate(k, d, src, dst, sem):
        at = (z + d) % n_z
        return remote(src.at[span(k), at], dst.at[span(k), at], sem, mr.at[k], mate * ratio + y, col)

    def send_box(k, d, src, dst, sem):
        at = (z + d) % n_z
        return remote(src.at[span(k), at], dst.at[z // 2, span(k)], sem, br.at[k], row_z(d), col)

    def send_h(k, d):
        return remote(last.at[span(k), (y + d) % ratio], ry.at[d - 1, span(k)], hs.at[d - 1], ur.at[d - 1, k], row_y(d), col)

    def send_u(k, d):
        return remote(sums.at[span(k), :, (y + d) % ratio], turn_in.at[d - 1, span(k)], us.at[d - 1], ur.at[d - 1, k], row_y(d), col)

    def send_s(k, d):
        return remote(thin.at[span(k), (z + d) % n_z], straight_in.at[d - 1, span(k)], ds, br.at[k], row_z(d), col)

    home = z == col

    load_w = pltpu.make_async_copy(w_hbm, w_v, in_sem.at[0])
    load_obs = pltpu.make_async_copy(obs_hbm, obs_v, in_sem.at[1])
    load_own = pltpu.make_async_copy(own, v1.at[:, col], own_sem)
    load_raw = pltpu.make_async_copy(raw_hbm, raw, in_sem.at[2])
    load_flags = pltpu.make_async_copy(flags_hbm, flags, in_sem.at[3])
    load_mask = pltpu.make_async_copy(mask_hbm, mask, in_sem.at[4])
    load_raw.start()
    load_flags.start()

    barrier = pltpu.get_barrier_semaphore()

    def tell(to_row, to_col):
        pl.semaphore_signal(barrier, inc=1, device_id=(to_row, to_col), device_id_type=MESH)

    @pl.when(jnp.logical_not(home))
    def _():
        for j in range(n_col):
            tell(col * ratio + y, j)

    @pl.when(home)
    def _():
        for d in range(1, ratio):
            for j in range(n_col):
                tell(row_y(d), j)

    for d in range(1, n_z):
        tell(row_z(d), col)
    for d in range(1, ratio):
        tell(row_y(d), col)
    for d in range(1, n_col):
        tell(row, (col + d) % n_col)

    load_raw.wait()
    load_flags.wait()
    load_mask.start()
    load_w.start()
    load_obs.start()
    flag_value = flags[...].astype(jnp.float32)
    flag_both = jnp.concatenate([flag_value, flag_value], axis=1)
    flagged = raw[...].astype(jnp.float32) * flag_both[:, None, :]
    own[...] = jnp.transpose(flagged, (1, 0, 2)).astype(jnp.bfloat16)
    load_own.start()
    pl.semaphore_wait(barrier, n_col - 1 + 2 * (n_z - 1) + 2 * (ratio - 1))

    @pl.loop(0, chunks)
    def _(k):
        for d in range(1, n_x):
            send_x(k, d).start()
        for d in range(n_z - 1, 0, -1):
            @pl.when(d <= z)
            def _():
                send_z(k, d).start()
        for d in range(n_z - 1, 0, -1):
            @pl.when(d > z)
            def _():
                send_z(k, d).start()
        for d in range(1, ratio):
            send_home(k, d).start()
        send_own(k).start()

    load_own.wait()

    def pass_first(k):
        got = v1.at[span(k), pl.ds(0, n_x - 1)]
        pltpu.make_async_copy(got, got, xr.at[k]).wait()
        for d in range(1, n_x):
            send_on(k, d).start()

    def wait_first(k):
        got = v1.at[span(k), pl.ds(0, n_x)]
        pltpu.make_async_copy(got, got, fr.at[k]).wait()

    def local_copy(k):
        return pltpu.make_async_copy(v1.at[span(k)], v2.at[span(k), y], lz)

    lane = lax.broadcasted_iota(jnp.int32, (1, 2 * half), 1)
    low_plus = jnp.where(lane < half, 1.0, -1.0).astype(jnp.float32)

    def compute(f):
        a = v1[f].astype(jnp.float32).reshape(first_rows, 2 * half)
        b = v2[f].astype(jnp.float32).reshape(second_rows, 2 * half).astype(jnp.bfloat16)
        turned = pltpu.roll(a, half, 1) * low_plus
        w = jnp.concatenate([a, turned], axis=0).astype(jnp.bfloat16)
        cross = lax.dot_general(w, b, (((1,), (1,)), ((), ())), preferred_element_type=jnp.float32)
        scale = mask[...].astype(jnp.float32) * w_v[f].astype(jnp.float32)
        res = jnp.concatenate(
            [
                (scale * (cross[:first_rows] - obs_v[0, f].astype(jnp.float32))).astype(jnp.bfloat16),
                (scale * (cross[first_rows:] - obs_v[1, f].astype(jnp.float32))).astype(jnp.bfloat16),
            ],
            axis=0,
        )
        t = jnp.dot(res, b, preferred_element_type=jnp.float32)
        g1 = t[:first_rows] - pltpu.roll(t[first_rows:], half, 1) * low_plus
        gf[f] = g1.reshape(n_x, 2, shard, 2 * half).astype(jnp.bfloat16)
        g2 = lax.dot_general(res, w, (((0,), (0,)), ((), ())), preferred_element_type=jnp.float32)
        sums[f] = g2.reshape(n_z, ratio, shard, 2 * half).astype(jnp.bfloat16)

    def wide(ref, *at):
        return ref[at].astype(jnp.float32)

    def to_mate(k, src, dst, sem):
        @pl.when(outer)
        def _():
            for d in range(1, n_z):
                send_mate(k, d, src, dst, sem).start()

    def fold(k, src, got, total, box, sem):
        @pl.when(jnp.logical_not(outer))
        def _():
            all_of = got.at[span(k), pl.ds(0, n_z - 1)]
            pltpu.make_async_copy(all_of, all_of, mr.at[k]).wait()
            total[span(k), mate] = src[span(k), mate]
            for d in range(1, n_z):
                at = (mate + d) % n_z
                total[span(k), at] = (wide(src, span(k), at) + wide(got, span(k), at)).astype(jnp.bfloat16)
            for d in range(1, n_z):
                send_box(k, d, total, box, sem).start()

    def unfold(k, src, total, box, put):
        pairs = n_z // 2

        def boxes(count):
            all_of = box.at[pl.ds(0, count), span(k)]
            pltpu.make_async_copy(all_of, all_of, br.at[k]).wait()

        @pl.when(outer)
        def _():
            boxes(pairs)
            out = wide(src, span(k), z)
            for m in range(pairs):
                out = out + wide(box, m, span(k))
            put(out.astype(jnp.bfloat16))

        @pl.when(jnp.logical_not(outer))
        def _():
            if pairs > 1:
                boxes(pairs - 1)
            out = wide(total, span(k), z)
            for m in range(1, pairs):
                out = out + wide(box, (z // 2 + m) % pairs, span(k))
            put(out.astype(jnp.bfloat16))

    def second_stage(k, step):
        plain = jnp.logical_not(jnp.logical_or(z_first(k), straight(k)))

        def put_last(value):
            last[span(k)] = value
            for d in range(1, ratio):
                send_h(k, d).start()

        def put_out(value):
            out_second[span(k)] = value

        @pl.when(z_first(k))
        def _():
            if step == 0:
                fold(k, sums, got_wide, total_wide, box_wide, zw)
            elif step == 1:
                unfold(k, sums, total_wide, box_wide, put_last)
            else:
                total = wide(last, span(k), y)
                for d in range(1, ratio):
                    send_h(k, d).wait_recv()
                    total = total + wide(ry, d - 1, span(k))
                put_out(total.astype(jnp.bfloat16))

        if step == 0:
            @pl.when(jnp.logical_not(z_first(k)))
            def _():
                total = wide(sums, span(k), slice(None), y)
                for d in range(1, ratio):
                    send_u(k, d).wait_recv()
                    total = total + wide(turn_in, d - 1, span(k))
                thin[span(k)] = total.astype(jnp.bfloat16)

                @pl.when(straight(k))
                def _():
                    for d in range(1, n_z):
                        send_s(k, d).start()

                @pl.when(jnp.logical_not(straight(k)))
                def _():
                    to_mate(k, thin, got_thin, zt)
        else:
            @pl.when(plain)
            def _():
                if step == 1:
                    fold(k, thin, got_thin, total_thin, box_thin, zt)
                else:
                    unfold(k, thin, total_thin, box_thin, put_out)

        if step == 1:
            @pl.when(straight(k))
            def _():
                got = straight_in.at[:, span(k)]
                pltpu.make_async_copy(got, got, br.at[k]).wait()
                total = wide(thin, span(k), z)
                for d in range(1, n_z):
                    total = total + wide(straight_in, d - 1, span(k))
                put_out(total.astype(jnp.bfloat16))

    lag_y = LAG_Y
    lag_c = lag_y + LAG_C
    lag_p = lag_c + LAG_P
    lag_s, at = [], lag_y
    for step in range(3):
        at = at + LAG_STAGES[min(step, len(LAG_STAGES) - 1)]
        lag_s.append(at)

    def sent(ref, sem, count=chunks):
        if count:
            got = ref.at[pl.ds(0, count * group)]
            pltpu.make_async_copy(got, got, sem).wait()

    early = sum(k in Z_FIRST for k in range(chunks))
    last_ones = sum(k in STRAIGHT for k in range(chunks))

    def gather_sent():
        sent(v1.at[:, pl.ds(0, n_col - 1)], fs)
        pltpu.make_async_copy(straight_in, straight_in, zs).wait()
        for d in range(1, ratio):
            sent(own, hy.at[d - 1])

            @pl.when(jnp.logical_not(home))
            def _():
                sent(v1, ys.at[d - 1])

    def sums_sent():
        sent(rc, cs)
        sent(got_wide.at[:, pl.ds(0, n_z - 1)], zw, early)
        for d in range(1, ratio):
            sent(own, hs.at[d - 1], early)
            sent(turn_in.at[d - 1], us.at[d - 1], chunks - early)

    last_wide = max([k for k in range(chunks) if k in Z_FIRST], default=0)
    sums_done = max(chunks + lag_c, last_wide + lag_s[1] + 1)

    @pl.loop(0, chunks + max(lag_s[-1], lag_p))
    def _(it):
        @pl.when(it == chunks + lag_y + 1)
        def _():
            gather_sent()

        @pl.when(it == sums_done + 1)
        def _():
            sums_sent()

        @pl.when(it < chunks)
        def _():
            @pl.when(jnp.logical_not(home))
            def _():
                got = v2.at[span(it), y]
                pltpu.make_async_copy(got, got, zr.at[it]).wait()
                for d in range(1, ratio):
                    send_y(it, d).start()

        @pl.when(jnp.logical_and(it >= LAG_F, it < chunks + LAG_F))
        def _():
            pass_first(it - LAG_F)

        @pl.when(jnp.logical_and(it >= lag_y, it < chunks + lag_y))
        def _():
            k = it - lag_y

            @pl.when(k == 0)
            def _():
                load_mask.wait()
                load_w.wait()
                load_obs.wait()

            for d in range(1, ratio):
                send_y(k, d).wait_recv()

            wait_first(k)

            @pl.when(home)
            def _():
                local_copy(k).start()
                local_copy(k).wait()

            for i in range(group):
                compute(k * group + i)

            @pl.when(z_first(k))
            def _():
                to_mate(k, sums, got_wide, zw)

            @pl.when(jnp.logical_not(z_first(k)))
            def _():
                for d in range(1, ratio):
                    send_u(k, d).start()

            send_c(k).start()

        for step in range(3):
            @pl.when(jnp.logical_and(it >= lag_s[step], it < chunks + lag_s[step]))
            def _():
                second_stage(it - lag_s[step], step)

        def full_block(lag):
            return jnp.logical_and(jnp.logical_and(it >= lag, it < chunks + lag), (it - lag) % block == block - 1)

        @pl.when(full_block(lag_c))
        def _():
            b = (it - lag_c) // block
            at = wide_span(b)
            got = rc.at[at]
            pltpu.make_async_copy(got, got, cr.at[b]).wait()
            gf_sum[at] = (wide(gf, at, slice(None), core) + wide(rc, at)).astype(jnp.bfloat16)
            for d in range(1, n_x):
                send_p(b, d).start()

        @pl.when(full_block(lag_p))
        def _():
            b = (it - lag_p) // block
            at = wide_span(b)
            total = wide(gf_sum, at, x)
            for d in range(1, n_x):
                send_p(b, d).wait_recv()
                total = total + wide(rx, d - 1, at)
            out_first[at] = total.astype(jnp.bfloat16)

    sent(got_thin.at[:, pl.ds(0, n_z - 1)], zt, chunks - early - last_ones)
    if last_ones:
        all_of = straight_in.at[:, pl.ds(0, last_ones * group)]
        pltpu.make_async_copy(all_of, all_of, ds).wait()
    for d in range(1, n_x):
        sent(own, ps.at[d - 1])


def turn_kernel(first, second, out_first, out_second):
    for src, dst in ((first, out_first), (second, out_second)):
        dst[...] = jnp.transpose(src[...].astype(jnp.float32), (1, 0, 2)).astype(jnp.bfloat16)


def per_device(n_row, n_col, spectra, window_flags, pair_mask, misfit_weight, observed):
    shard, freqs, width = spectra.shape
    ratio = n_row // n_col
    n_z, n_x = n_row // ratio, n_col // 2
    group = GROUP if freqs % GROUP == 0 else 1
    chunks = freqs // group
    bf = jnp.bfloat16
    vm = lambda *shape: pltpu.VMEM(shape, bf)
    dma = lambda *shape: pltpu.SemaphoreType.DMA(shape)
    one = pltpu.SemaphoreType.DMA
    blocks = chunks // BLOCK if chunks % BLOCK == 0 else chunks
    first, second = pl.pallas_call(
        functools.partial(kernel, n_row, n_col, chunks, group),
        out_shape=[pltpu.VMEM((freqs, shard, width), bf)] * 2,
        in_specs=[
            pl.BlockSpec(memory_space=pl.ANY),
        ] * 5,
        out_specs=[pl.BlockSpec(memory_space=pltpu.VMEM)] * 2,
        scratch_shapes=[
            pltpu.VMEM(spectra.shape, bf),
            pltpu.VMEM(window_flags.shape, window_flags.dtype),
            pltpu.VMEM(pair_mask.shape, pair_mask.dtype),
            vm(freqs, shard, width),
            vm(freqs, n_col, shard, width),
            vm(freqs, ratio, n_col, shard, width),
            pltpu.VMEM(misfit_weight.shape, bf),
            pltpu.VMEM(observed.shape, bf),
            vm(freqs, n_x, 2, shard, width),
            vm(freqs, n_x, shard, width),
            vm(freqs, n_x, shard, width),
            vm(n_x - 1, freqs, shard, width),
            vm(freqs, n_z, ratio, shard, width),
            vm(freqs, n_z, ratio, shard, width),
            vm(freqs, n_z, ratio, shard, width),
            vm(n_z // 2, freqs, ratio, shard, width),
            vm(freqs, ratio, shard, width),
            vm(ratio - 1, freqs, shard, width),
            vm(ratio - 1, freqs, n_z, shard, width),
            vm(freqs, n_z, shard, width),
            vm(freqs, n_z, shard, width),
            vm(freqs, n_z, shard, width),
            vm(n_z // 2, freqs, shard, width),
            vm(n_z - 1, freqs, shard, width),
            dma(5), pltpu.SemaphoreType.DMA,
            dma(chunks), one, dma(chunks),
            one, dma(chunks), one, dma(ratio - 1),
            dma(ratio - 1), dma(ratio - 1, chunks),
            one, dma(blocks), dma(n_x - 1), dma(n_x - 1, blocks),
            dma(ratio - 1), dma(ratio - 1), dma(ratio - 1, chunks),
            one, one, dma(chunks), dma(chunks), one,
        ],
        compiler_params=pltpu.CompilerParams(collective_id=0, has_side_effects=True),
        name="adjoint",
    )(spectra, window_flags, pair_mask, misfit_weight, observed)
    first, second = pl.pallas_call(
        turn_kernel,
        out_shape=[jax.ShapeDtypeStruct((shard, freqs, width), bf)] * 2,
        in_specs=[pl.BlockSpec(memory_space=pltpu.VMEM)] * 2,
        out_specs=[pl.BlockSpec(memory_space=pltpu.VMEM)] * 2,
        name="turn",
    )(*(pltpu.with_memory_space_constraint(part, pltpu.VMEM) for part in (first, second)))
    return first, second[None]


def solution(mesh):
    placed = (
        P(("row", "col"), None, None),
        P(("row", "col"), None),
        P("row", "col"),
        P(None, "row", "col"),
        P(None, None, "row", "col"),
    )
    return jax.shard_map(
        functools.partial(per_device, mesh.shape["row"], mesh.shape["col"]),
        mesh=mesh,
        in_specs=placed,
        out_specs=(P(("row", "col"), None, None), P("col", "row", None, None)),
        check_vma=False,
    )
```

```python
import functools

import jax
import jax.numpy as jnp
from jax import lax
from jax.experimental import pallas as pl
from jax.experimental.pallas import tpu as pltpu
from jax.sharding import PartitionSpec as P

MESH = pl.DeviceIdType.MESH
GROUP = 2
LAG_Y = 4
LAG_STAGES = (4, 4, 4)
LAG_C, LAG_P = 3, 5
Z_FIRST = (0, 1, 2, 3)
STRAIGHT = (6, 7)
LAG_F = 0
BLOCK = 8


def among(k, some):
    yes = k < 0
    for one in some:
        yes = jnp.logical_or(yes, k == one)
    return yes


def z_first(k):
    return among(k, Z_FIRST)


def straight(k):
    return among(k, STRAIGHT)


def kernel(
    n_row, n_col, chunks, group,
    raw_hbm, flags_hbm, mask_hbm, w_hbm, obs_hbm, out_first, out_second,
    raw, flags, mask, own,
    v1, v2, w_v, obs_v, gf, gf_sum, rc, rx, sums, got_wide, total_wide, box_wide, last, ry, turn_in, thin, got_thin, total_thin, box_thin, straight_in,
    in_sem, own_sem, xr, fs, fr, zs, zr, lz, hy, ys, yr,
    cs, cr, ps, pr, hs, us, ur, zw, zt, mr, br, ds,
):
    ratio = n_row // n_col
    n_z = n_row // ratio
    n_x = n_col // 2
    row, col = lax.axis_index("row"), lax.axis_index("col")
    z, y = row // ratio, row % ratio
    x, core = col // 2, col % 2
    shard = own.shape[1]
    first_rows = n_col * shard
    second_rows = ratio * first_rows
    half = own.shape[2] // 2

    def col_at(step):
        return ((x + step) % n_x) * 2 + core

    partner = x * 2 + (1 - core)

    def row_y(step):
        return z * ratio + (y + step) % ratio

    def row_z(step):
        return ((z + step) % n_z) * ratio + y

    block = BLOCK if chunks % BLOCK == 0 else 1

    def wide_span(b):
        return pl.ds(b * block * group, block * group)

    def span(k):
        return pl.ds(k * group, group)

    def remote(src, dst, ssem, rsem, to_row, to_col):
        return pltpu.make_async_remote_copy(
            src_ref=src, dst_ref=dst, send_sem=ssem, recv_sem=rsem,
            device_id=(to_row, to_col), device_id_type=MESH,
        )

    def send_x(k, d):
        return remote(own.at[span(k)], v1.at[span(k), col], fs, xr.at[k], row, col_at(d))

    def send_own(k):
        return remote(own.at[span(k)], v1.at[span(k), col], fs, fr.at[k], row, partner)

    def send_on(k, d):
        got = v1.at[span(k), col_at(d)]
        return remote(got, got, fs, fr.at[k], row, partner)

    def send_z(k, d):
        to_z = jnp.where(d <= z, z - d, d)
        return remote(own.at[span(k)], v2.at[span(k), y, col], zs, zr.at[k], to_z * ratio + y, z)

    def send_home(k, d):
        return remote(own.at[span(k)], v2.at[span(k), y, col], hy.at[d - 1], yr.at[d - 1, k], row_y(d), z)

    def send_y(k, d):
        src = v2.at[span(k), y]
        return remote(src, src, ys.at[d - 1], yr.at[d - 1, k], row_y(d), col)

    def send_c(k):
        return remote(gf.at[span(k), :, 1 - core], rc.at[span(k)], cs, cr.at[k // block], row, partner)

    def send_p(b, d):
        at = wide_span(b)
        return remote(gf_sum.at[at, (x + d) % n_x], rx.at[d - 1, at], ps.at[d - 1], pr.at[d - 1, b], row, col_at(d))

    upper = (z // (n_z // 2)) % 2
    outer = z % 2 == upper
    mate = z + 1 - 2 * (z % 2)

    def send_mate(k, d, src, dst, sem):
        at = (z + d) % n_z
        return remote(src.at[span(k), at], dst.at[span(k), at], sem, mr.at[k], mate * ratio + y, col)

    def send_box(k, d, src, dst, sem):
        at = (z + d) % n_z
        return remote(src.at[span(k), at], dst.at[z // 2, span(k)], sem, br.at[k], row_z(d), col)

    def send_h(k, d):
        return remote(last.at[span(k), (y + d) % ratio], ry.at[d - 1, span(k)], hs.at[d - 1], ur.at[d - 1, k], row_y(d), col)

    def send_u(k, d):
        return remote(sums.at[span(k), :, (y + d) % ratio], turn_in.at[d - 1, span(k)], us.at[d - 1], ur.at[d - 1, k], row_y(d), col)

    def send_s(k, d):
        return remote(thin.at[span(k), (z + d) % n_z], straight_in.at[d - 1, span(k)], ds, br.at[k], row_z(d), col)

    home = z == col

    load_w = pltpu.make_async_copy(w_hbm, w_v, in_sem.at[0])
    load_obs = pltpu.make_async_copy(obs_hbm, obs_v, in_sem.at[1])
    load_own = pltpu.make_async_copy(own, v1.at[:, col], own_sem)
    load_raw = pltpu.make_async_copy(raw_hbm, raw, in_sem.at[2])
    load_flags = pltpu.make_async_copy(flags_hbm, flags, in_sem.at[3])
    load_mask = pltpu.make_async_copy(mask_hbm, mask, in_sem.at[4])
    load_raw.start()
    load_flags.start()

    barrier = pltpu.get_barrier_semaphore()

    def tell(to_row, to_col):
        pl.semaphore_signal(barrier, inc=1, device_id=(to_row, to_col), device_id_type=MESH)

    @pl.when(jnp.logical_not(home))
    def _():
        for j in range(n_col):
            tell(col * ratio + y, j)

    @pl.when(home)
    def _():
        for d in range(1, ratio):
            for j in range(n_col):
                tell(row_y(d), j)

    for d in range(1, n_z):
        tell(row_z(d), col)
    for d in range(1, ratio):
        tell(row_y(d), col)
    for d in range(1, n_col):
        tell(row, (col + d) % n_col)

    load_raw.wait()
    load_flags.wait()
    load_mask.start()
    load_w.start()
    load_obs.start()
    flag_value = flags[...].astype(jnp.float32)
    flag_both = jnp.concatenate([flag_value, flag_value], axis=1)
    flagged = raw[...].astype(jnp.float32) * flag_both[:, None, :]
    own[...] = jnp.transpose(flagged, (1, 0, 2)).astype(jnp.bfloat16)
    load_own.start()
    pl.semaphore_wait(barrier, n_col - 1 + 2 * (n_z - 1) + 2 * (ratio - 1))

    @pl.loop(0, chunks)
    def _(k):
        for d in range(1, n_x):
            send_x(k, d).start()
        for d in range(n_z - 1, 0, -1):
            @pl.when(d <= z)
            def _():
                send_z(k, d).start()
        for d in range(n_z - 1, 0, -1):
            @pl.when(d > z)
            def _():
                send_z(k, d).start()
        for d in range(1, ratio):
            send_home(k, d).start()
        send_own(k).start()

    load_own.wait()

    def pass_first(k):
        got = v1.at[span(k), pl.ds(0, n_x - 1)]
        pltpu.make_async_copy(got, got, xr.at[k]).wait()
        for d in range(1, n_x):
            send_on(k, d).start()

    def wait_first(k):
        got = v1.at[span(k), pl.ds(0, n_x)]
        pltpu.make_async_copy(got, got, fr.at[k]).wait()

    def local_copy(k):
        return pltpu.make_async_copy(v1.at[span(k)], v2.at[span(k), y], lz)

    lane = lax.broadcasted_iota(jnp.int32, (1, 2 * half), 1)
    low_plus = jnp.where(lane < half, 1.0, -1.0).astype(jnp.float32)

    def compute(f):
        a = v1[f].astype(jnp.float32).reshape(first_rows, 2 * half)
        b = v2[f].astype(jnp.float32).reshape(second_rows, 2 * half).astype(jnp.bfloat16)
        turned = pltpu.roll(a, half, 1) * low_plus
        w = jnp.concatenate([a, turned], axis=0).astype(jnp.bfloat16)
        cross = lax.dot_general(w, b, (((1,), (1,)), ((), ())), preferred_element_type=jnp.float32)
        scale = mask[...].astype(jnp.float32) * w_v[f].astype(jnp.float32)
        res = jnp.concatenate(
            [
                (scale * (cross[:first_rows] - obs_v[0, f].astype(jnp.float32))).astype(jnp.bfloat16),
                (scale * (cross[first_rows:] - obs_v[1, f].astype(jnp.float32))).astype(jnp.bfloat16),
            ],
            axis=0,
        )
        t = jnp.dot(res, b, preferred_element_type=jnp.float32)
        g1 = t[:first_rows] - pltpu.roll(t[first_rows:], half, 1) * low_plus
        gf[f] = g1.reshape(n_x, 2, shard, 2 * half).astype(jnp.bfloat16)
        g2 = lax.dot_general(res, w, (((0,), (0,)), ((), ())), preferred_element_type=jnp.float32)
        sums[f] = g2.reshape(n_z, ratio, shard, 2 * half).astype(jnp.bfloat16)

    def wide(ref, *at):
        return ref[at].astype(jnp.float32)

    def to_mate(k, src, dst, sem):
        @pl.when(outer)
        def _():
            for d in range(1, n_z):
                send_mate(k, d, src, dst, sem).start()

    def fold(k, src, got, total, box, sem):
        @pl.when(jnp.logical_not(outer))
        def _():
            all_of = got.at[span(k), pl.ds(0, n_z - 1)]
            pltpu.make_async_copy(all_of, all_of, mr.at[k]).wait()
            total[span(k), mate] = src[span(k), mate]
            for d in range(1, n_z):
                at = (mate + d) % n_z
                total[span(k), at] = (wide(src, span(k), at) + wide(got, span(k), at)).astype(jnp.bfloat16)
            for d in range(1, n_z):
                send_box(k, d, total, box, sem).start()

    def unfold(k, src, total, box, put):
        pairs = n_z // 2

        def boxes(count):
            all_of = box.at[pl.ds(0, count), span(k)]
            pltpu.make_async_copy(all_of, all_of, br.at[k]).wait()

        @pl.when(outer)
        def _():
            boxes(pairs)
            out = wide(src, span(k), z)
            for m in range(pairs):
                out = out + wide(box, m, span(k))
            put(out.astype(jnp.bfloat16))

        @pl.when(jnp.logical_not(outer))
        def _():
            if pairs > 1:
                boxes(pairs - 1)
            out = wide(total, span(k), z)
            for m in range(1, pairs):
                out = out + wide(box, (z // 2 + m) % pairs, span(k))
            put(out.astype(jnp.bfloat16))

    def second_stage(k, step):
        plain = jnp.logical_not(jnp.logical_or(z_first(k), straight(k)))

        def put_last(value):
            last[span(k)] = value
            for d in range(1, ratio):
                send_h(k, d).start()

        def put_out(value):
            out_second[span(k)] = value

        @pl.when(z_first(k))
        def _():
            if step == 0:
                fold(k, sums, got_wide, total_wide, box_wide, zw)
            elif step == 1:
                unfold(k, sums, total_wide, box_wide, put_last)
            else:
                total = wide(last, span(k), y)
                for d in range(1, ratio):
                    send_h(k, d).wait_recv()
                    total = total + wide(ry, d - 1, span(k))
                put_out(total.astype(jnp.bfloat16))

        if step == 0:
            @pl.when(jnp.logical_not(z_first(k)))
            def _():
                total = wide(sums, span(k), slice(None), y)
                for d in range(1, ratio):
                    send_u(k, d).wait_recv()
                    total = total + wide(turn_in, d - 1, span(k))
                thin[span(k)] = total.astype(jnp.bfloat16)

                @pl.when(straight(k))
                def _():
                    for d in range(1, n_z):
                        send_s(k, d).start()

                @pl.when(jnp.logical_not(straight(k)))
                def _():
                    to_mate(k, thin, got_thin, zt)
        else:
            @pl.when(plain)
            def _():
                if step == 1:
                    fold(k, thin, got_thin, total_thin, box_thin, zt)
                else:
                    unfold(k, thin, total_thin, box_thin, put_out)

        if step == 1:
            @pl.when(straight(k))
            def _():
                got = straight_in.at[:, span(k)]
                pltpu.make_async_copy(got, got, br.at[k]).wait()
                total = wide(thin, span(k), z)
                for d in range(1, n_z):
                    total = total + wide(straight_in, d - 1, span(k))
                put_out(total.astype(jnp.bfloat16))

    lag_y = LAG_Y
    lag_c = lag_y + LAG_C
    lag_p = lag_c + LAG_P
    lag_s, at = [], lag_y
    for step in range(3):
        at = at + LAG_STAGES[min(step, len(LAG_STAGES) - 1)]
        lag_s.append(at)

    def sent(ref, sem, count=chunks):
        if count:
            got = ref.at[pl.ds(0, count * group)]
            pltpu.make_async_copy(got, got, sem).wait()

    early = sum(k in Z_FIRST for k in range(chunks))
    last_ones = sum(k in STRAIGHT for k in range(chunks))

    def gather_sent():
        sent(v1.at[:, pl.ds(0, n_col - 1)], fs)
        pltpu.make_async_copy(straight_in, straight_in, zs).wait()
        for d in range(1, ratio):
            sent(own, hy.at[d - 1])

            @pl.when(jnp.logical_not(home))
            def _():
                sent(v1, ys.at[d - 1])

    def sums_sent():
        sent(rc, cs)
        sent(got_wide.at[:, pl.ds(0, n_z - 1)], zw, early)
        for d in range(1, ratio):
            sent(own, hs.at[d - 1], early)
            sent(turn_in.at[d - 1], us.at[d - 1], chunks - early)

    last_wide = max([k for k in range(chunks) if k in Z_FIRST], default=0)
    sums_done = max(chunks + lag_c, last_wide + lag_s[1] + 1)

    @pl.loop(0, chunks + max(lag_s[-1], lag_p))
    def _(it):
        @pl.when(it == chunks + lag_y + 1)
        def _():
            gather_sent()

        @pl.when(it == sums_done + 1)
        def _():
            sums_sent()

        @pl.when(it < chunks)
        def _():
            @pl.when(jnp.logical_not(home))
            def _():
                got = v2.at[span(it), y]
                pltpu.make_async_copy(got, got, zr.at[it]).wait()
                for d in range(1, ratio):
                    send_y(it, d).start()

        @pl.when(jnp.logical_and(it >= LAG_F, it < chunks + LAG_F))
        def _():
            pass_first(it - LAG_F)

        @pl.when(jnp.logical_and(it >= lag_y, it < chunks + lag_y))
        def _():
            k = it - lag_y

            @pl.when(k == 0)
            def _():
                load_mask.wait()
                load_w.wait()
                load_obs.wait()

            for d in range(1, ratio):
                send_y(k, d).wait_recv()

            wait_first(k)

            @pl.when(home)
            def _():
                local_copy(k).start()
                local_copy(k).wait()

            for i in range(group):
                compute(k * group + i)

            @pl.when(z_first(k))
            def _():
                to_mate(k, sums, got_wide, zw)

            @pl.when(jnp.logical_not(z_first(k)))
            def _():
                for d in range(1, ratio):
                    send_u(k, d).start()

            send_c(k).start()

        for step in range(3):
            @pl.when(jnp.logical_and(it >= lag_s[step], it < chunks + lag_s[step]))
            def _():
                second_stage(it - lag_s[step], step)

        def full_block(lag):
            return jnp.logical_and(jnp.logical_and(it >= lag, it < chunks + lag), (it - lag) % block == block - 1)

        @pl.when(full_block(lag_c))
        def _():
            b = (it - lag_c) // block
            at = wide_span(b)
            got = rc.at[at]
            pltpu.make_async_copy(got, got, cr.at[b]).wait()
            gf_sum[at] = (wide(gf, at, slice(None), core) + wide(rc, at)).astype(jnp.bfloat16)
            for d in range(1, n_x):
                send_p(b, d).start()

        @pl.when(full_block(lag_p))
        def _():
            b = (it - lag_p) // block
            at = wide_span(b)
            total = wide(gf_sum, at, x)
            for d in range(1, n_x):
                send_p(b, d).wait_recv()
                total = total + wide(rx, d - 1, at)
            out_first[at] = total.astype(jnp.bfloat16)

    sent(got_thin.at[:, pl.ds(0, n_z - 1)], zt, chunks - early - last_ones)
    if last_ones:
        all_of = straight_in.at[:, pl.ds(0, last_ones * group)]
        pltpu.make_async_copy(all_of, all_of, ds).wait()
    for d in range(1, n_x):
        sent(own, ps.at[d - 1])


def turn_kernel(first, second, out_first, out_second):
    for src, dst in ((first, out_first), (second, out_second)):
        dst[...] = jnp.transpose(src[...].astype(jnp.float32), (1, 0, 2)).astype(jnp.bfloat16)


def per_device(n_row, n_col, spectra, window_flags, pair_mask, misfit_weight, observed):
    shard, freqs, width = spectra.shape
    ratio = n_row // n_col
    n_z, n_x = n_row // ratio, n_col // 2
    group = GROUP if freqs % GROUP == 0 else 1
    chunks = freqs // group
    bf = jnp.bfloat16
    vm = lambda *shape: pltpu.VMEM(shape, bf)
    dma = lambda *shape: pltpu.SemaphoreType.DMA(shape)
    one = pltpu.SemaphoreType.DMA
    blocks = chunks // BLOCK if chunks % BLOCK == 0 else chunks
    first, second = pl.pallas_call(
        functools.partial(kernel, n_row, n_col, chunks, group),
        out_shape=[pltpu.VMEM((freqs, shard, width), bf)] * 2,
        in_specs=[
            pl.BlockSpec(memory_space=pl.ANY),
        ] * 5,
        out_specs=[pl.BlockSpec(memory_space=pltpu.VMEM)] * 2,
        scratch_shapes=[
            pltpu.VMEM(spectra.shape, bf),
            pltpu.VMEM(window_flags.shape, window_flags.dtype),
            pltpu.VMEM(pair_mask.shape, pair_mask.dtype),
            vm(freqs, shard, width),
            vm(freqs, n_col, shard, width),
            vm(freqs, ratio, n_col, shard, width),
            pltpu.VMEM(misfit_weight.shape, bf),
            pltpu.VMEM(observed.shape, bf),
            vm(freqs, n_x, 2, shard, width),
            vm(freqs, n_x, shard, width),
            vm(freqs, n_x, shard, width),
            vm(n_x - 1, freqs, shard, width),
            vm(freqs, n_z, ratio, shard, width),
            vm(freqs, n_z, ratio, shard, width),
            vm(freqs, n_z, ratio, shard, width),
            vm(n_z // 2, freqs, ratio, shard, width),
            vm(freqs, ratio, shard, width),
            vm(ratio - 1, freqs, shard, width),
            vm(ratio - 1, freqs, n_z, shard, width),
            vm(freqs, n_z, shard, width),
            vm(freqs, n_z, shard, width),
            vm(freqs, n_z, shard, width),
            vm(n_z // 2, freqs, shard, width),
            vm(n_z - 1, freqs, shard, width),
            dma(5), pltpu.SemaphoreType.DMA,
            dma(chunks), one, dma(chunks),
            one, dma(chunks), one, dma(ratio - 1),
            dma(ratio - 1), dma(ratio - 1, chunks),
            one, dma(blocks), dma(n_x - 1), dma(n_x - 1, blocks),
            dma(ratio - 1), dma(ratio - 1), dma(ratio - 1, chunks),
            one, one, dma(chunks), dma(chunks), one,
        ],
        compiler_params=pltpu.CompilerParams(collective_id=0, has_side_effects=True),
        name="adjoint",
    )(spectra, window_flags, pair_mask, misfit_weight, observed)
    first, second = pl.pallas_call(
        turn_kernel,
        out_shape=[jax.ShapeDtypeStruct((shard, freqs, width), bf)] * 2,
        in_specs=[pl.BlockSpec(memory_space=pltpu.VMEM)] * 2,
        out_specs=[pl.BlockSpec(memory_space=pltpu.VMEM)] * 2,
        name="turn",
    )(*(pltpu.with_memory_space_constraint(part, pltpu.VMEM) for part in (first, second)))
    return first, second[None]


def solution(mesh):
    placed = (
        P(("row", "col"), None, None),
        P(("row", "col"), None),
        P("row", "col"),
        P(None, "row", "col"),
        P(None, None, "row", "col"),
    )
    return jax.shard_map(
        functools.partial(per_device, mesh.shape["row"], mesh.shape["col"]),
        mesh=mesh,
        in_specs=placed,
        out_specs=(P(("row", "col"), None, None), P("col", "row", None, None)),
        check_vma=False,
    )
```
